256 devices in a mesh: dp: 32 (over z, x_hi, core), depth: 8 (over y, x_lo).
Axes of the slice: x: 4 (x_hi: 2, x_lo: 2; x = x_hi * 2 + x_lo), y: 4, z: 8, core: 2. Of those that a mesh axis runs over, the one named last changes fastest.
Arguments:
- volume: bfloat16 [32, 4, 16, 8, 128], P('dp', None, 'depth'), may hold values from -6 to 6
- kernel_one: bfloat16 [32, 4, 3, 3, 3], replicated, may hold values from -0.625 to 0.625
- bias_one: float32 [32], replicated, may hold values from -0.5 to 0.5
- kernel_two: bfloat16 [64, 32, 3, 3, 3], replicated, may hold values from -0.21875 to 0.21875
- bias_two: float32 [64], replicated, may hold values from -0.5 to 0.5
- cotangent: bfloat16 [32, 64, 16, 8, 128], P('dp', None, 'depth'), may hold values from -0.008239746 to 0.008239746
Outputs:
- features: bfloat16 [32, 64, 16, 8, 128], P('dp', None, 'depth')
- grad_kernel_one: float32 [32, 4, 3, 3, 3], replicated
- grad_bias_one: float32 [32], replicated
- grad_kernel_two: float32 [64, 32, 3, 3, 3], replicated
- grad_bias_two: float32 [64], replicated
The draws below stay inside these ranges and needn't reach their ends.
All inputs are finite; a program needn't handle non-finite values.
Results may differ from the reference program's by a relative error of at most 0.006.
Values may be sent and summed in bfloat16 or wider, within the bound.
No kernel may reach another device: no remote copies, remote signals or barrier semaphores. Data moves between devices by JAX's collectives and lax.ppermute only.
A program may use at most 64 MiB of HBM per device.

```python
import jax
import jax.numpy as jnp
from jax import lax

C_IN = 4
C_ONE = 32
C_TWO = 64
HY = 8
HX = 128
SAMPLES = 32
NZ = 16


def level_of(rng, shape, shards, least, high):
    def one(position, blocks):
        steps = jax.random.uniform(jax.random.fold_in(jax.random.fold_in(rng, 6), position), (blocks,), jnp.float32, least / len(shards), high / len(shards))
        return jnp.repeat(jnp.exp(steps), shape[position] // blocks).reshape((-1,) + (1,) * (len(shape) - position - 1))

    level = one(*shards[0])
    for cut in shards[1:]:
        level = level * one(*cut)
    return level


def noise(stream_key, shape, scale, bound, shards=(), held_as=jnp.bfloat16):
    drawn = jax.random.normal(stream_key, shape, jnp.float32) * scale
    if len(shards) > 0:
        drawn = level_of(stream_key, shape, shards, -0.22, 0.18) * drawn
    return jnp.clip(drawn, min=-bound, max=bound).astype(held_as)


def setup_inputs(seed: int = 0) -> dict:
    streams_of = jax.random.split(jax.random.key(seed), 7)
    return {
        "volume": noise(streams_of[0], (SAMPLES, C_IN, NZ, HY, HX), 1.0, 6.0, ((0, 32), (2, 8))),
        "kernel_one": noise(streams_of[1], (C_ONE, C_IN, 3, 3, 3), (27 * C_IN) ** -0.5, 0.625),
        "bias_one": jnp.clip(jax.random.uniform(streams_of[2], (C_ONE,), jnp.float32, -0.5, 0.5), -0.5, 0.5),
        "kernel_two": noise(streams_of[3], (C_TWO, C_ONE, 3, 3, 3), (27 * C_ONE) ** -0.5, 0.21875),
        "bias_two": jnp.clip(jax.random.uniform(streams_of[4], (C_TWO,), jnp.float32, -0.5, 0.5), -0.5, 0.5),
        "cotangent": noise(streams_of[5], (SAMPLES, C_TWO, NZ, HY, HX), (1.0 / (SAMPLES * NZ * HY * HX) ** 0.5), 0.008239746, ((0, 32), (2, 8))),
    }


FORWARD_DIMS = ('NCDHW', 'OIDHW', 'NCDHW')
KERNEL_DIMS = ('CNDHW', 'IODHW', 'CNDHW')

def convolve(inputs, kernel):
    return lax.conv_general_dilated(inputs.astype(jnp.float32), kernel.astype(jnp.float32), (1, 1, 1), ((1, 1), (1, 1), (1, 1)), dimension_numbers=FORWARD_DIMS, precision=lax.Precision.HIGHEST)

def kernel_grad(inputs, slope):
    return lax.conv_general_dilated(inputs.astype(jnp.float32), slope.astype(jnp.float32), (1, 1, 1), ((1, 1), (1, 1), (1, 1)), dimension_numbers=KERNEL_DIMS, precision=lax.Precision.HIGHEST)

def silu_slope(value):
    sig = jax.nn.sigmoid(value)
    return sig * (1.0 + value * (1.0 - sig))

def reference(volume, kernel_one, bias_one, kernel_two, bias_two, cotangent):
    flipped = jnp.transpose(jnp.flip(kernel_two, (2, 3, 4)), (1, 0, 2, 3, 4))

    def one_sample(carry, pieces):
        sample, upstream = pieces
        sample = sample[None]
        upstream = upstream[None]
        pre_one = convolve(sample, kernel_one) + bias_one[None, :, None, None, None]
        act_one = jax.nn.silu(pre_one).astype(jnp.bfloat16)
        pre_two = convolve(act_one, kernel_two) + bias_two[None, :, None, None, None]
        feature = jax.nn.silu(pre_two).astype(jnp.bfloat16)
        slope_two = (upstream.astype(jnp.float32) * silu_slope(pre_two)).astype(jnp.bfloat16)
        grad_two = kernel_grad(act_one, slope_two)
        bias_grad_two = lax.optimization_barrier(jnp.sum(slope_two.astype(jnp.float32), axis=(0, 2, 3, 4)))
        back_one = convolve(slope_two, flipped)
        slope_one = (back_one * silu_slope(pre_one)).astype(jnp.bfloat16)
        grad_one = kernel_grad(sample, slope_one)
        bias_grad_one = lax.optimization_barrier(jnp.sum(slope_one.astype(jnp.float32), axis=(0, 2, 3, 4)))
        carry = (carry[0] + grad_one, carry[1] + bias_grad_one, carry[2] + grad_two, carry[3] + bias_grad_two)
        return (carry, feature[0])
    start = (jnp.zeros(kernel_one.shape, jnp.float32), jnp.zeros(bias_one.shape, jnp.float32), jnp.zeros(kernel_two.shape, jnp.float32), jnp.zeros(bias_two.shape, jnp.float32))
    totals, features = lax.scan(one_sample, start, (volume, cotangent))
    return (features, totals[0], totals[1], totals[2], totals[3])
```

```python
import jax
import jax.numpy as jnp
from jax import lax
from jax.sharding import Mesh
from jax.sharding import PartitionSpec as P

DP = ("z", "x_hi", "core")
DEPTH = ("y", "x_lo")
PLANE = ("x_hi", "core", "y", "x_lo")
LINE = "z"
FORWARD_DIMS = ("NCDHW", "OIDHW", "NCDHW")
KERNEL_DIMS = ("CNDHW", "IODHW", "CNDHW")


def extended(x, sides, width):
    for axis, dim in sides:
        size, length = (lax.axis_size(axis), x.shape[dim])
        up = [(i, (i + 1) % size) for i in range(size - 1)]
        down = [(j, i) for i, j in up]
        last = lax.slice_in_dim(x, length - width, length, axis=dim)
        leading = lax.slice_in_dim(x, 0, width, axis=dim)
        before = lax.ppermute(last, axis, up)
        after = lax.ppermute(leading, axis, down)
        x = jnp.concatenate([before, x, after], axis=dim)
    return x


def convolve(inputs, kernel, depth_pad=0):
    return lax.conv_general_dilated(
        inputs,
        kernel,
        (1, 1, 1),
        ((depth_pad, depth_pad), (1, 1), (1, 1)),
        dimension_numbers=FORWARD_DIMS,
        preferred_element_type=jnp.float32,
    )


def kernel_grad(inputs, slope):
    return lax.conv_general_dilated(
        inputs,
        slope,
        (1, 1, 1),
        ((0, 0), (1, 1), (1, 1)),
        dimension_numbers=KERNEL_DIMS,
        preferred_element_type=jnp.float32,
    )


def silu_slope(value):
    sig = jax.nn.sigmoid(value)
    return sig * (1.0 + value * (1.0 - sig))


def exchange(x, axes):
    return lax.all_to_all(x, axes, 0, 0, tiled=True)


def reduced(x):
    rows, lanes = x.shape
    plane = lax.axis_size(PLANE)
    line = lax.axis_size(LINE)
    part = exchange(x.reshape(plane, rows // plane, lanes), PLANE)
    part = jnp.sum(part, axis=0, dtype=jnp.float32).astype(x.dtype)
    part = exchange(jnp.broadcast_to(part[None], (line,) + part.shape), LINE)
    part = jnp.sum(part, axis=0, dtype=jnp.float32).astype(x.dtype)
    part = exchange(jnp.broadcast_to(part[None], (plane,) + part.shape), PLANE)
    return part.reshape(rows, lanes)


def per_device(volume, kernel_one, bias_one, kernel_two, bias_two, cotangent):
    planes = volume.shape[2]
    shift_one = bias_one[None, :, None, None, None]
    padded = extended(volume, ((DEPTH, 2),), 2)
    pre_wide = convolve(padded, kernel_one) + shift_one
    global_plane = lax.axis_index(DEPTH) * planes + jnp.arange(planes + 2, dtype=jnp.int32) - 1
    inside = (global_plane >= 0) & (global_plane < planes * lax.axis_size(DEPTH))
    inside = inside.astype(jnp.float32)[None, None, :, None, None]
    act_wide = (jax.nn.silu(pre_wide) * inside).astype(jnp.bfloat16)
    pre_one = pre_wide[:, :, 1:-1]
    input_wide = padded[:, :, 1:-1]
    pre_two = convolve(act_wide, kernel_two) + bias_two[None, :, None, None, None]
    features = jax.nn.silu(pre_two).astype(jnp.bfloat16)
    slope_two = (cotangent.astype(jnp.float32) * silu_slope(pre_two)).astype(jnp.bfloat16)
    grad_two = kernel_grad(act_wide, slope_two)
    bias_grad_two = jnp.sum(slope_two, axis=(0, 2, 3, 4), dtype=jnp.float32)
    flipped = jnp.transpose(jnp.flip(kernel_two, (2, 3, 4)), (1, 0, 2, 3, 4))
    slope_wide = extended(slope_two, ((DEPTH, 2),), 1)
    back_one = convolve(slope_wide, flipped)
    slope_one = (back_one * silu_slope(pre_one)).astype(jnp.bfloat16)
    grad_one = kernel_grad(input_wide, slope_one)
    bias_grad_one = jnp.sum(slope_one, axis=(0, 2, 3, 4), dtype=jnp.float32)
    two = jnp.transpose(grad_two, (2, 3, 4, 1, 0)).reshape(432, 128)
    one = jnp.transpose(grad_one, (2, 3, 4, 1, 0)).reshape(27, 128)
    biases = jnp.concatenate([bias_grad_one, bias_grad_two, jnp.zeros((32,), jnp.float32)]).reshape(1, 128)
    packed = jnp.concatenate([two, one, biases, jnp.zeros((52, 128), jnp.float32)])
    total = reduced(packed.astype(jnp.bfloat16)).astype(jnp.float32)
    grad_two = jnp.transpose(total[:432].reshape(3, 3, 3, 32, 64), (4, 3, 0, 1, 2))
    grad_one = jnp.transpose(total[432:459].reshape(3, 3, 3, 4, 32), (4, 3, 0, 1, 2))
    return (features, grad_one, total[459, :32], grad_two, total[459, 32:96])


def solution(mesh):
    cut = Mesh(mesh.devices.reshape(8, 2, 2, 4, 2), DP + DEPTH)
    return jax.shard_map(
        per_device,
        mesh=cut,
        in_specs=(
            P(DP, None, DEPTH, None, None),
            P(),
            P(),
            P(),
            P(),
            P(DP, None, DEPTH, None, None),
        ),
        out_specs=(P(DP, None, DEPTH, None, None), P(), P(), P(), P()),
        check_vma=False,
    )
```

```python
import jax
import jax.numpy as jnp
from jax import lax
from jax.experimental import pallas as pl
from jax.experimental.pallas import tpu as pltpu
from jax.sharding import Mesh
from jax.sharding import PartitionSpec as P

DP = ("z", "x_hi", "core")
DEPTH = ("y", "x_lo")
PLANE = ("x_hi", "core", "y", "x_lo")
LINE = "z"

BF = jnp.bfloat16
F32 = jnp.float32
HY = 8
HX = 128
CELLS = HY * HX
ROWS = HY + 1
C_IN = 4
C_ONE = 32
C_TWO = 64
V_PITCH = 72
C_PITCH = 40
F_PITCH = 24


def dot_nn(a, b):
    return lax.dot_general(a, b, (((1,), (0,)), ((), ())), preferred_element_type=F32)


def dot_nt(a, b):
    return lax.dot_general(a, b, (((1,), (1,)), ((), ())), preferred_element_type=F32)


def identity(n):
    return lax.broadcasted_iota(jnp.int32, (n, n), 0) == lax.broadcasted_iota(jnp.int32, (n, n), 1)


def column(row):
    n = row.shape[1]
    return jnp.sum(jnp.where(identity(n), jnp.broadcast_to(row, (n, n)), 0.0), axis=1, keepdims=True)


def transposed(w):
    return dot_nt(identity(w.shape[1]).astype(BF), w).astype(BF)


def sigmoid(v):
    return 1.0 / (1.0 + jnp.exp(-v))


def neighbours(x):
    lane = lax.broadcasted_iota(jnp.int32, x.shape, 1)
    before = jnp.where(lane == 0, 0.0, pltpu.roll(x, 1, 1))
    after = jnp.where(lane == HX - 1, 0.0, pltpu.roll(x, HX - 1, 1))
    return before, x, after


def compute(
    depth, vm2, vm1, v0, vp1, vp2, w1, b1, w2, b2, cm, c0, cp,
    features, packed,
    vs, x1, x1b, x3, s3, cs, fs, w1s, p1, pk,
):
    sources = ((vm2, 1), (vm1, 0), (vm1, 1), (v0, 0), (v0, 1), (vp1, 0), (vp1, 1), (vp2, 0))
    for p, (ref, z) in enumerate(sources):
        for i in range(C_IN):
            vs[i * V_PITCH + p * HY : i * V_PITCH + (p + 1) * HY, :] = ref[0, i, z].astype(F32)
    row_id = lax.broadcasted_iota(jnp.int32, (12, HX), 0)
    x1[36:48, :] = jnp.where(lax.broadcasted_iota(jnp.int32, (12, 8 * CELLS), 0) == 0, 1.0, 0.0)
    for p in range(8):
        x1[0:12, p * CELLS : p * CELLS + HX] = jnp.zeros((12, HX), F32)
        x1[24:36, p * CELLS + 7 * HX : (p + 1) * CELLS] = jnp.zeros((12, HX), F32)
        for y in range(HY):
            slab = vs[pl.ds(p * HY + y, C_IN, stride=V_PITCH), :]
            for c, moved in enumerate(neighbours(slab)):
                for b in range(3):
                    to = y + 1 - b
                    if 0 <= to < HY:
                        col = p * CELLS + to * HX
                        x1[b * 12 + c * 4 : b * 12 + c * 4 + 4, col : col + HX] = moved
        x1b[:, p * CELLS : (p + 1) * CELLS] = x1[:, p * CELLS : (p + 1) * CELLS].astype(BF)
    w1s[...] = jnp.zeros((144, C_ONE), F32)
    for a in range(3):
        for t in range(9):
            w1s[a * 48 + t * 4 : a * 48 + t * 4 + 4, :] = w1[a * 9 + t].astype(F32)
    w1t = [transposed(w1s[a * 48 : (a + 1) * 48, :].astype(BF)) for a in range(3)]
    bias1 = column(b1[...])
    bias2 = column(b2[...])
    for p in range(7):
        x3[:, p * ROWS * HX : p * ROWS * HX + HX] = jnp.zeros((96, HX), BF)
    for q in range(5):
        s3[:, q * ROWS * HX : q * ROWS * HX + HX] = jnp.zeros((192, HX), BF)
    first = depth[0] * 2 - 2
    for p in range(6):
        pre = bias1 + sum(dot_nn(w1t[a], x1b[:, (p + a) * CELLS : (p + a + 1) * CELLS]) for a in range(3))
        sig = sigmoid(pre)
        if p in (2, 3):
            p1[:, (p - 2) * CELLS : (p - 1) * CELLS] = sig * (1.0 + pre * (1.0 - sig))
        inside = jnp.logical_and(first + p >= 0, first + p < 16)
        act = pre * sig * jnp.where(inside, 1.0, 0.0)
        for y in range(HY):
            col = (1 + p * ROWS + y) * HX
            for c, moved in enumerate(neighbours(act[:, y * HX : (y + 1) * HX])):
                x3[c * C_ONE : (c + 1) * C_ONE, col : col + HX] = moved.astype(BF)
    for q, (ref, z) in enumerate(((cm, 0), (c0, 0), (c0, 1), (cp, 0))):
        for o in range(C_TWO):
            cs[o * C_PITCH + q * HY : o * C_PITCH + (q + 1) * HY, :] = ref[0, o, z].astype(F32)
    w2t = [transposed(w2[3 * k : 3 * k + 3].reshape(96, C_TWO)) for k in range(9)]
    for q in range(4):
        pre = bias2
        for k in range(9):
            col = ((q + k // 3) * ROWS + k % 3) * HX
            pre = pre + dot_nn(w2t[k], x3[:, col : col + CELLS])
        sig = sigmoid(pre)
        slope = sig * (1.0 + pre * (1.0 - sig))
        act = pre * sig
        for y in range(HY):
            cot = cs[pl.ds(q * HY + y, C_TWO, stride=C_PITCH), :]
            here = (cot * slope[:, y * HX : (y + 1) * HX]).astype(BF).astype(F32)
            col = (1 + q * ROWS + y) * HX
            for c, moved in enumerate(neighbours(here)):
                s3[c * C_TWO : (c + 1) * C_TWO, col : col + HX] = moved.astype(BF)
            if q in (1, 2):
                fs[pl.ds((q - 1) * HY + y, C_TWO, stride=F_PITCH), :] = act[:, y * HX : (y + 1) * HX]
    for o in range(C_TWO):
        for z in range(2):
            features[0, o, z] = fs[o * F_PITCH + z * HY : o * F_PITCH + (z + 1) * HY, :].astype(BF)
    mine = [s3[C_TWO : 2 * C_TWO, (1 + q * ROWS) * HX : (1 + q * ROWS) * HX + CELLS] for q in (1, 2)]
    pk[384:512, :] = jnp.zeros((128, HX), F32)
    for k in range(9):
        grad = 0.0
        for j in range(2):
            col = ((1 + j + k // 3) * ROWS + k % 3) * HX
            grad = grad + dot_nt(x3[:, col : col + CELLS], mine[j])
        pk[(k % 4) * 96 if k < 8 else 384 : (k % 4) * 96 + 96 if k < 8 else 480, (k // 4 % 2) * 64 : (k // 4 % 2) * 64 + 64] = grad
    ones = jnp.ones((8, CELLS), BF)
    bias_two = dot_nt(ones, mine[0]) + dot_nt(ones, mine[1])
    pk[480:488, 0:64] = bias_two
    flipped = []
    for k in range(9):
        flipped.append(jnp.concatenate([w2[(8 - k) * 3 + 2 - c] for c in range(3)], axis=1))
    ones_grad = []
    for j in range(2):
        back = 0.0
        for k in range(9):
            col = ((j + k // 3) * ROWS + k % 3) * HX
            back = back + dot_nn(flipped[k], s3[:, col : col + CELLS])
        slope1 = (back * p1[:, j * CELLS : (j + 1) * CELLS]).astype(BF)
        ones_grad.append([dot_nt(x1b[:, (2 + j + a) * CELLS : (3 + j + a) * CELLS], slope1) for a in range(3)])
    for a in range(3):
        grad = ones_grad[0][a] + ones_grad[1][a]
        pk[384 + a * 40 : 384 + a * 40 + 40, 64:96] = grad[:40]
    packed[...] = pk[...].astype(BF).reshape(32, 16, HX)


def unpack(total, two, one, bias_one, bias_two):
    flat = total[...].astype(F32).reshape(512, HX)
    for k in range(9):
        r = (k % 4) * 96 if k < 8 else 384
        lane = (k // 4 % 2) * 64
        two[3 * k : 3 * k + 3] = flat[r : r + 96, lane : lane + 64].reshape(3, C_ONE, C_TWO)
    for a in range(3):
        for t in range(9):
            r = 384 + a * 40 + t * 4
            one[a * 9 + t] = flat[r : r + 4, 64:96]
    bias_one[...] = flat[384 + 36 : 384 + 37, 64:96]
    bias_two[...] = flat[480:481, 0:64]


def exchange(x, axes):
    return lax.all_to_all(x, axes, 0, 0, tiled=True)


def reduced(x):
    plane = lax.axis_size(PLANE)
    line = lax.axis_size(LINE)
    part = exchange(x, PLANE)
    part = jnp.sum(part, axis=0, dtype=F32).astype(x.dtype)
    part = exchange(jnp.broadcast_to(part[None], (line,) + part.shape), LINE)
    part = jnp.sum(part, axis=0, dtype=F32).astype(x.dtype)
    return exchange(jnp.broadcast_to(part[None], (plane,) + part.shape), PLANE)


def shifted(x, step):
    size = lax.axis_size(DEPTH)
    pairs = [(i, i + step) for i in range(size) if 0 <= i + step < size]
    return lax.ppermute(x, DEPTH, pairs)


VMEM = pl.BlockSpec(memory_space=pltpu.VMEM)
SMEM = pl.BlockSpec(memory_space=pltpu.SMEM)


def local(depth, volumes, w1, b1, w2, b2, cots, interpret=False):
    return pl.pallas_call(
        compute,
        out_shape=(
            jax.ShapeDtypeStruct((1, C_TWO, 2, HY, HX), BF),
            jax.ShapeDtypeStruct((32, 16, HX), BF),
        ),
        in_specs=[SMEM] + [VMEM] * 12,
        out_specs=(VMEM, VMEM),
        scratch_shapes=[
            pltpu.VMEM((C_IN * V_PITCH, HX), F32),
            pltpu.VMEM((48, 8 * CELLS), F32),
            pltpu.VMEM((48, 8 * CELLS), BF),
            pltpu.VMEM((96, 55 * HX), BF),
            pltpu.VMEM((192, 37 * HX), BF),
            pltpu.VMEM((C_TWO * C_PITCH, HX), F32),
            pltpu.VMEM((C_TWO * F_PITCH, HX), F32),
            pltpu.VMEM((144, C_ONE), F32),
            pltpu.VMEM((C_ONE, 2 * CELLS), F32),
            pltpu.VMEM((512, HX), F32),
        ],
        compiler_params=pltpu.CompilerParams(vmem_limit_bytes=48 * 1024 * 1024),
        interpret=interpret,
        name="slab",
    )(depth, *volumes, w1, b1, w2, b2, *cots)


def split(total, interpret=False):
    return pl.pallas_call(
        unpack,
        out_shape=(
            jax.ShapeDtypeStruct((27, C_ONE, C_TWO), F32),
            jax.ShapeDtypeStruct((27, C_IN, C_ONE), F32),
            jax.ShapeDtypeStruct((1, C_ONE), F32),
            jax.ShapeDtypeStruct((1, C_TWO), F32),
        ),
        in_specs=[VMEM],
        out_specs=(VMEM,) * 4,
        interpret=interpret,
        name="unpack",
    )(total)


def per_device(volume, kernel_one, bias_one, kernel_two, bias_two, cotangent):
    volumes = (shifted(volume, 2), shifted(volume, 1), volume, shifted(volume, -1), shifted(volume, -2))
    cots = (shifted(cotangent[:, :, 1:], 1), cotangent, shifted(cotangent[:, :, :1], -1))
    depth = lax.axis_index(DEPTH).astype(jnp.int32).reshape(1)
    w1 = jnp.transpose(kernel_one, (2, 3, 4, 1, 0)).reshape(27, C_IN, C_ONE)
    w2 = jnp.transpose(kernel_two, (2, 3, 4, 1, 0)).reshape(27, C_ONE, C_TWO)
    features, packed = local(depth, volumes, w1, bias_one[None], w2, bias_two[None], cots)
    two, one, b1, b2 = split(reduced(packed))
    two = jnp.transpose(two.reshape(3, 3, 3, C_ONE, C_TWO), (4, 3, 0, 1, 2))
    one = jnp.transpose(one.reshape(3, 3, 3, C_IN, C_ONE), (4, 3, 0, 1, 2))
    return (features, one, b1[0], two, b2[0])


def solution(mesh):
    cut = Mesh(mesh.devices.reshape(8, 2, 2, 4, 2), DP + DEPTH)
    return jax.shard_map(
        per_device,
        mesh=cut,
        in_specs=(
            P(DP, None, DEPTH, None, None),
            P(),
            P(),
            P(),
            P(),
            P(DP, None, DEPTH, None, None),
        ),
        out_specs=(P(DP, None, DEPTH, None, None), P(), P(), P(), P()),
        check_vma=False,
    )
```

```python
import jax
import jax.numpy as jnp
from jax import lax
from jax.experimental import pallas as pl
from jax.experimental.pallas import tpu as pltpu
from jax.sharding import Mesh
from jax.sharding import PartitionSpec as P

DP = ("z", "x_hi", "core")
DEPTH = ("y", "x_lo")
PLANE = ("x_hi", "core", "y", "x_lo")
LINE = "z"

BF = jnp.bfloat16
F32 = jnp.float32
HY = 8
HX = 128
CELLS = HY * HX
ROWS = HY + 1
C_IN = 4
C_ONE = 32
C_TWO = 64
V_PITCH = 56
C_PITCH = 24


def dot_nn(a, b):
    return lax.dot_general(a, b, (((1,), (0,)), ((), ())), preferred_element_type=F32)


def dot_nt(a, b):
    return lax.dot_general(a, b, (((1,), (1,)), ((), ())), preferred_element_type=F32)


def identity(n):
    return lax.broadcasted_iota(jnp.int32, (n, n), 0) == lax.broadcasted_iota(jnp.int32, (n, n), 1)


def column(row):
    n = row.shape[1]
    return jnp.sum(jnp.where(identity(n), jnp.broadcast_to(row, (n, n)), 0.0), axis=1, keepdims=True)


def transposed(w):
    return dot_nt(identity(w.shape[1]).astype(BF), w).astype(BF)


def sigmoid(v):
    return 1.0 / (1.0 + jnp.exp(-v))


def neighbours(x):
    lane = lax.broadcasted_iota(jnp.int32, x.shape, 1)
    before = jnp.where(lane == 0, 0.0, pltpu.roll(x, 1, 1))
    after = jnp.where(lane == HX - 1, 0.0, pltpu.roll(x, HX - 1, 1))
    return before, x, after


def compute(
    depth, va, v0, vb, w1, b1, w2, b2, c0,
    features, packed,
    vs, x1, x1b, x3, s3, cs, fs, w1s, p1, pk,
):
    even = depth[0] % 2 == 0
    for p in range(6):
        for i in range(C_IN):
            if p in (2, 3):
                plane = v0[0, i, p % 2].astype(F32)
            else:
                near = va[0, i, p % 2].astype(F32)
                far = vb[0, i, p % 2].astype(F32)
                plane = jnp.where(even, far, near) if p < 2 else jnp.where(even, near, far)
            vs[i * V_PITCH + p * HY : i * V_PITCH + (p + 1) * HY, :] = plane
    x1[36:48, :] = jnp.where(lax.broadcasted_iota(jnp.int32, (12, 6 * CELLS), 0) == 0, 1.0, 0.0)
    for p in range(6):
        x1[0:12, p * CELLS : p * CELLS + HX] = jnp.zeros((12, HX), F32)
        x1[24:36, p * CELLS + 7 * HX : (p + 1) * CELLS] = jnp.zeros((12, HX), F32)
        for y in range(HY):
            slab = vs[pl.ds(p * HY + y, C_IN, stride=V_PITCH), :]
            for c, moved in enumerate(neighbours(slab)):
                for b in range(3):
                    to = y + 1 - b
                    if 0 <= to < HY:
                        col = p * CELLS + to * HX
                        x1[b * 12 + c * 4 : b * 12 + c * 4 + 4, col : col + HX] = moved
        x1b[:, p * CELLS : (p + 1) * CELLS] = x1[:, p * CELLS : (p + 1) * CELLS].astype(BF)
    w1s[...] = jnp.zeros((144, C_ONE), F32)
    for a in range(3):
        for t in range(9):
            w1s[a * 48 + t * 4 : a * 48 + t * 4 + 4, :] = w1[a * 9 + t].astype(F32)
    w1t = [transposed(w1s[a * 48 : (a + 1) * 48, :].astype(BF)) for a in range(3)]
    bias1 = column(b1[...])
    bias2 = column(b2[...])
    for p in range(5):
        x3[:, p * ROWS * HX : p * ROWS * HX + HX] = jnp.zeros((96, HX), BF)
    for q in range(3):
        s3[:, q * ROWS * HX : q * ROWS * HX + HX] = jnp.zeros((192, HX), BF)
    for p in range(4):
        pre = bias1 + sum(dot_nn(w1t[a], x1b[:, (p + a) * CELLS : (p + a + 1) * CELLS]) for a in range(3))
        sig = sigmoid(pre)
        slope = sig * (1.0 + pre * (1.0 - sig))
        act = pre * sig
        if p in (0, 3):
            inside = jnp.where(depth[0] > 0 if p == 0 else depth[0] < depth[1] - 1, 1.0, 0.0)
            slope = slope * inside
            act = act * inside
        p1[:, p * CELLS : (p + 1) * CELLS] = slope
        for y in range(HY):
            col = (1 + p * ROWS + y) * HX
            for c, moved in enumerate(neighbours(act[:, y * HX : (y + 1) * HX])):
                x3[c * C_ONE : (c + 1) * C_ONE, col : col + HX] = moved.astype(BF)
    for z in range(2):
        for o in range(C_TWO):
            cs[o * C_PITCH + z * HY : o * C_PITCH + (z + 1) * HY, :] = c0[0, o, z].astype(F32)
    w2t = [transposed(w2[3 * k : 3 * k + 3].reshape(96, C_TWO)) for k in range(9)]
    for q in range(2):
        pre = bias2
        for k in range(9):
            col = ((q + k // 3) * ROWS + k % 3) * HX
            pre = pre + dot_nn(w2t[k], x3[:, col : col + CELLS])
        sig = sigmoid(pre)
        slope = sig * (1.0 + pre * (1.0 - sig))
        act = pre * sig
        for y in range(HY):
            row = q * HY + y
            cot = cs[pl.ds(row, C_TWO, stride=C_PITCH), :]
            here = (cot * slope[:, y * HX : (y + 1) * HX]).astype(BF).astype(F32)
            col = (1 + q * ROWS + y) * HX
            for c, moved in enumerate(neighbours(here)):
                s3[c * C_TWO : (c + 1) * C_TWO, col : col + HX] = moved.astype(BF)
            fs[pl.ds(row, C_TWO, stride=C_PITCH), :] = act[:, y * HX : (y + 1) * HX]
    for o in range(C_TWO):
        for z in range(2):
            features[0, o, z] = fs[o * C_PITCH + z * HY : o * C_PITCH + (z + 1) * HY, :].astype(BF)
    mine = [s3[C_TWO : 2 * C_TWO, (1 + q * ROWS) * HX : (1 + q * ROWS) * HX + CELLS] for q in range(2)]
    pk[384:512, :] = jnp.zeros((128, HX), F32)
    for k in range(9):
        grad = 0.0
        for j in range(2):
            col = ((j + k // 3) * ROWS + k % 3) * HX
            grad = grad + dot_nt(x3[:, col : col + CELLS], mine[j])
        row, lane = place(k)
        pk[row : row + 96, lane : lane + C_TWO] = grad
    ones = jnp.ones((8, CELLS), BF)
    pk[480:488, 0:C_TWO] = dot_nt(ones, mine[0]) + dot_nt(ones, mine[1])
    flipped = []
    for k in range(9):
        flipped.append(jnp.concatenate([w2[(8 - k) * 3 + 2 - c] for c in range(3)], axis=1))
    grads = [0.0, 0.0, 0.0]
    for t in range(4):
        back = 0.0
        for k in range(9):
            j = t + k // 3 - 2
            if 0 <= j < 2:
                col = (j * ROWS + k % 3) * HX
                back = back + dot_nn(flipped[k], s3[:, col : col + CELLS])
        share = back * p1[:, t * CELLS : (t + 1) * CELLS]
        high = share.astype(BF)
        share = jnp.concatenate([high, (share - high.astype(F32)).astype(BF)], axis=0)
        for a in range(3):
            grads[a] = grads[a] + dot_nt(x1b[:, (t + a) * CELLS : (t + a + 1) * CELLS], share)
    for a in range(3):
        grad = grads[a][:40]
        pk[384 + a * 40 : 384 + a * 40 + 40, C_TWO : C_TWO + C_ONE] = grad[:, :C_ONE] + grad[:, C_ONE:]
    packed[...] = pk[...].astype(BF).reshape(32, 16, HX)


def place(k):
    return ((k % 4) * 96, (k // 4) * C_TWO) if k < 8 else (384, 0)


def unpack(total, two, one, bias_one, bias_two):
    flat = total[...].astype(F32).reshape(512, HX)
    for k in range(9):
        r, lane = place(k)
        two[3 * k : 3 * k + 3] = flat[r : r + 96, lane : lane + 64].reshape(3, C_ONE, C_TWO)
    for a in range(3):
        for t in range(9):
            r = 384 + a * 40 + t * 4
            one[a * 9 + t] = flat[r : r + 4, 64:96]
    bias_one[...] = flat[384 + 36 : 384 + 37, 64:96]
    bias_two[...] = flat[480:481, 0:64]


def exchange(x, axes):
    return lax.all_to_all(x, axes, 0, 0, tiled=True)


def reduced(x):
    plane = lax.axis_size(PLANE)
    line = lax.axis_size(LINE)
    part = exchange(x, PLANE)
    part = jnp.sum(part, axis=0, dtype=F32).astype(x.dtype)
    part = exchange(jnp.broadcast_to(part[None], (line,) + part.shape), LINE)
    part = jnp.sum(part, axis=0, dtype=F32).astype(x.dtype)
    return exchange(jnp.broadcast_to(part[None], (plane,) + part.shape), PLANE)


def swapped(x, first):
    size = lax.axis_size(DEPTH)
    ups = [(i, i + 1) for i in range(first, size - 1, 2)]
    return lax.ppermute(x, DEPTH, ups + [(j, i) for i, j in ups])


VMEM = pl.BlockSpec(memory_space=pltpu.VMEM)
SMEM = pl.BlockSpec(memory_space=pltpu.SMEM)


def local(depth, volumes, w1, b1, w2, b2, cot, interpret=False):
    return pl.pallas_call(
        compute,
        out_shape=(
            jax.ShapeDtypeStruct((1, C_TWO, 2, HY, HX), BF),
            jax.ShapeDtypeStruct((32, 16, HX), BF),
        ),
        in_specs=[SMEM] + [VMEM] * 8,
        out_specs=(VMEM, VMEM),
        scratch_shapes=[
            pltpu.VMEM((C_IN * V_PITCH, HX), F32),
            pltpu.VMEM((48, 6 * CELLS), F32),
            pltpu.VMEM((48, 6 * CELLS), BF),
            pltpu.VMEM((96, 37 * HX), BF),
            pltpu.VMEM((192, 19 * HX), BF),
            pltpu.VMEM((C_TWO * C_PITCH, HX), F32),
            pltpu.VMEM((C_TWO * C_PITCH, HX), F32),
            pltpu.VMEM((144, C_ONE), F32),
            pltpu.VMEM((C_ONE, 4 * CELLS), F32),
            pltpu.VMEM((512, HX), F32),
        ],
        compiler_params=pltpu.CompilerParams(vmem_limit_bytes=48 * 1024 * 1024),
        interpret=interpret,
        name="slab",
    )(depth, *volumes, w1, b1, w2, b2, cot)


def split(total, interpret=False):
    return pl.pallas_call(
        unpack,
        out_shape=(
            jax.ShapeDtypeStruct((27, C_ONE, C_TWO), F32),
            jax.ShapeDtypeStruct((27, C_IN, C_ONE), F32),
            jax.ShapeDtypeStruct((1, C_ONE), F32),
            jax.ShapeDtypeStruct((1, C_TWO), F32),
        ),
        in_specs=[VMEM],
        out_specs=(VMEM,) * 4,
        interpret=interpret,
        name="unpack",
    )(total)


def per_device(volume, kernel_one, bias_one, kernel_two, bias_two, cotangent):
    volumes = (swapped(volume, 0), volume, swapped(volume, 1))
    depth = jnp.stack([lax.axis_index(DEPTH), lax.axis_size(DEPTH)]).astype(jnp.int32)
    w1 = jnp.transpose(kernel_one, (2, 3, 4, 1, 0)).reshape(27, C_IN, C_ONE)
    w2 = jnp.transpose(kernel_two, (2, 3, 4, 1, 0)).reshape(27, C_ONE, C_TWO)
    features, packed = local(depth, volumes, w1, bias_one[None], w2, bias_two[None], cotangent)
    two, one, b1, b2 = split(reduced(packed))
    two = jnp.transpose(two.reshape(3, 3, 3, C_ONE, C_TWO), (4, 3, 0, 1, 2))
    one = jnp.transpose(one.reshape(3, 3, 3, C_IN, C_ONE), (4, 3, 0, 1, 2))
    return (features, one, b1[0], two, b2[0])


def solution(mesh):
    cut = Mesh(mesh.devices.reshape(8, 2, 2, 4, 2), DP + DEPTH)
    return jax.shard_map(
        per_device,
        mesh=cut,
        in_specs=(
            P(DP, None, DEPTH, None, None),
            P(),
            P(),
            P(),
            P(),
            P(DP, None, DEPTH, None, None),
        ),
        out_specs=(P(DP, None, DEPTH, None, None), P(), P(), P(), P()),
        check_vma=False,
    )
```

```python
import jax
import jax.numpy as jnp
from jax import lax
from jax.experimental import pallas as pl
from jax.experimental.pallas import tpu as pltpu
from jax.sharding import Mesh
from jax.sharding import PartitionSpec as P

DP = ("z", "x_hi", "core")
DEPTH = ("y", "x_lo")
PLANE = ("x_hi", "core", "y", "x_lo")
LINE = "z"

BF = jnp.bfloat16
F32 = jnp.float32
HY = 8
HX = 128
CELLS = HY * HX
ROWS = HY + 1
C_IN = 4
C_ONE = 32
C_TWO = 64
V_PITCH = 56
C_PITCH = 24


def dot_nn(a, b):
    return lax.dot_general(a, b, (((1,), (0,)), ((), ())), preferred_element_type=F32)


def dot_nt(a, b):
    return lax.dot_general(a, b, (((1,), (1,)), ((), ())), preferred_element_type=F32)


def identity(n):
    return lax.broadcasted_iota(jnp.int32, (n, n), 0) == lax.broadcasted_iota(jnp.int32, (n, n), 1)


def column(row):
    n = row.shape[1]
    return jnp.sum(jnp.where(identity(n), jnp.broadcast_to(row, (n, n)), 0.0), axis=1, keepdims=True)


def transposed(w):
    return dot_nt(identity(w.shape[1]).astype(BF), w).astype(BF)


def sigmoid(v):
    return 1.0 / (1.0 + jnp.exp(-v))


def neighbours(x):
    lane = lax.broadcasted_iota(jnp.int32, x.shape, 1)
    before = jnp.where(lane == 0, 0.0, pltpu.roll(x, 1, 1))
    after = jnp.where(lane == HX - 1, 0.0, pltpu.roll(x, HX - 1, 1))
    return before, x, after


def prepare(w1, b1, w2, b2, c0, w1t, w2t, flip, bias, cot, w1v, w2v, cv, bv1, bv2, w1s, cs, sems):
    copies = [
        pltpu.make_async_copy(src, dst, sems.at[n])
        for n, (src, dst) in enumerate(((w1, w1v), (w2, w2v), (b1, bv1), (b2, bv2), (c0, cv)))
    ]
    for copy in copies:
        copy.start()
    w1s[...] = jnp.zeros((144, C_ONE), F32)
    copies[0].wait()
    for a in range(3):
        for t in range(9):
            w1s[a * 48 + t * 4 : a * 48 + t * 4 + 4, :] = w1v[a * 9 + t].astype(F32)
        w1t[a * C_ONE : (a + 1) * C_ONE, :] = transposed(w1s[a * 48 : (a + 1) * 48, :].astype(BF))
    copies[1].wait()
    for k in range(9):
        w2t[k * C_TWO : (k + 1) * C_TWO, :] = transposed(w2v[3 * k : 3 * k + 3].reshape(96, C_TWO))
        flip[k * C_ONE : (k + 1) * C_ONE, :] = jnp.concatenate([w2v[(8 - k) * 3 + 2 - c] for c in range(3)], axis=1)
    copies[2].wait()
    copies[3].wait()
    bias[0:C_ONE, :] = jnp.broadcast_to(column(bv1[...]), (C_ONE, HX))
    bias[C_ONE:, :] = jnp.broadcast_to(column(bv2[...]), (C_TWO, HX))
    copies[4].wait()
    for o in range(C_TWO):
        for z in range(2):
            cs[o * C_PITCH + z * HY : o * C_PITCH + (z + 1) * HY, :] = cv[0, o, z].astype(F32)
    for row in range(2 * HY):
        cot[:, row * HX : (row + 1) * HX] = cs[pl.ds(row, C_TWO, stride=C_PITCH), :].astype(BF)


def compute(
    depth, va, v0, vb, w1t, w2t, flip, bias, cot,
    features, packed,
    vs, x1, x1b, x3, s3, sb, fs, fb, p1, rs, pk, sem,
):
    even = depth[0] % 2 == 0
    for p in range(6):
        for i in range(C_IN):
            if p in (2, 3):
                plane = v0[0, i, p % 2].astype(F32)
            else:
                near = va[0, i, p % 2].astype(F32)
                far = vb[0, i, p % 2].astype(F32)
                plane = jnp.where(even, far, near) if p < 2 else jnp.where(even, near, far)
            vs[i * V_PITCH + p * HY : i * V_PITCH + (p + 1) * HY, :] = plane
    x1[36:48, :] = jnp.where(lax.broadcasted_iota(jnp.int32, (12, 6 * CELLS), 0) == 0, 1.0, 0.0)
    for p in range(6):
        x1[0:12, p * CELLS : p * CELLS + HX] = jnp.zeros((12, HX), F32)
        x1[24:36, p * CELLS + 7 * HX : (p + 1) * CELLS] = jnp.zeros((12, HX), F32)
        for y in range(HY):
            slab = vs[pl.ds(p * HY + y, C_IN, stride=V_PITCH), :]
            for c, moved in enumerate(neighbours(slab)):
                for b in range(3):
                    to = y + 1 - b
                    if 0 <= to < HY:
                        col = p * CELLS + to * HX
                        x1[b * 12 + c * 4 : b * 12 + c * 4 + 4, col : col + HX] = moved
        x1b[:, p * CELLS : (p + 1) * CELLS] = x1[:, p * CELLS : (p + 1) * CELLS].astype(BF)
    for p in range(5):
        x3[:, p * ROWS * HX : p * ROWS * HX + HX] = jnp.zeros((96, HX), BF)
    for p in range(4):
        pre = bias[0:C_ONE, 0:1]
        for a in range(3):
            pre = pre + dot_nn(w1t[a * C_ONE : (a + 1) * C_ONE, :], x1b[:, (p + a) * CELLS : (p + a + 1) * CELLS])
        sig = sigmoid(pre)
        slope = sig * (1.0 + pre * (1.0 - sig))
        act = pre * sig
        if p in (0, 3):
            inside = jnp.where(depth[0] > 0 if p == 0 else depth[0] < depth[1] - 1, 1.0, 0.0)
            slope = slope * inside
            act = act * inside
        p1[:, p * CELLS : (p + 1) * CELLS] = slope
        for y in range(HY):
            col = (1 + p * ROWS + y) * HX
            for c, moved in enumerate(neighbours(act[:, y * HX : (y + 1) * HX])):
                x3[c * C_ONE : (c + 1) * C_ONE, col : col + HX] = moved.astype(BF)
    for q in range(2):
        sb[0:C_TWO, q * CELLS + 7 * HX : (q + 1) * CELLS] = jnp.zeros((C_TWO, HX), BF)
        sb[2 * C_TWO :, q * CELLS : q * CELLS + HX] = jnp.zeros((C_TWO, HX), BF)
        pre = bias[C_ONE:, 0:1]
        for k in range(9):
            col = ((q + k // 3) * ROWS + k % 3) * HX
            pre = pre + dot_nn(w2t[k * C_TWO : (k + 1) * C_TWO, :], x3[:, col : col + CELLS])
        sig = sigmoid(pre)
        slope = sig * (1.0 + pre * (1.0 - sig))
        act = pre * sig
        for y in range(HY):
            row = q * HY + y
            col = row * HX
            up = cot[:, col : col + HX].astype(F32)
            here = (up * slope[:, y * HX : (y + 1) * HX]).astype(BF)
            for b in range(3):
                to = y + b - 1
                if 0 <= to < HY:
                    sb[b * C_TWO : (b + 1) * C_TWO, q * CELLS + to * HX : q * CELLS + (to + 1) * HX] = here
            for c, moved in enumerate(neighbours(here.astype(F32))):
                s3[c * C_TWO : (c + 1) * C_TWO, col : col + HX] = moved.astype(BF)
            fs[pl.ds(row, C_TWO, stride=C_PITCH), :] = act[:, y * HX : (y + 1) * HX]
    for o in range(C_TWO):
        for z in range(2):
            fb[0, o, z] = fs[o * C_PITCH + z * HY : o * C_PITCH + (z + 1) * HY, :].astype(BF)
    out = pltpu.make_async_copy(fb, features, sem)
    out.start()
    for j in range(2):
        rs[:, j * CELLS : (j + 1) * CELLS] = dot_nn(flip[...], s3[:, j * CELLS : (j + 1) * CELLS])
    pk[384:512, :] = jnp.zeros((128, HX), F32)
    for a in range(3):
        grad = 0.0
        for j in range(2):
            col = (1 + (j + a) * ROWS) * HX
            grad = grad + dot_nt(x3[:, col : col + CELLS], sb[:, j * CELLS : (j + 1) * CELLS])
        for b in range(3):
            row, lane = place(a * 3 + b)
            pk[row : row + 96, lane : lane + C_TWO] = grad[:, b * C_TWO : (b + 1) * C_TWO]
    ones = jnp.ones((8, 2 * CELLS), BF)
    pk[480:488, 0:C_TWO] = dot_nt(ones, s3[C_TWO : 2 * C_TWO, :])
    grads = 0.0
    for t in range(4):
        shares = []
        for y in range(HY):
            back = 0.0
            for k in range(9):
                j, row = t + k // 3 - 2, y + k % 3 - 1
                if 0 <= j < 2 and 0 <= row < HY:
                    col = j * CELLS + row * HX
                    back = back + rs[k * C_ONE : (k + 1) * C_ONE, col : col + HX]
            shares.append(back * p1[:, t * CELLS + y * HX : t * CELLS + (y + 1) * HX])
        share = jnp.concatenate(shares, axis=1)
        high = share.astype(BF)
        share = jnp.concatenate([high, (share - high.astype(F32)).astype(BF)], axis=0)
        near = jnp.concatenate([x1b[:, (t + a) * CELLS : (t + a + 1) * CELLS] for a in range(3)], axis=0)
        grads = grads + dot_nt(near, share)
    for a in range(3):
        grad = grads[a * 48 : a * 48 + 40]
        pk[384 + a * 40 : 384 + a * 40 + 40, C_TWO : C_TWO + C_ONE] = grad[:, :C_ONE] + grad[:, C_ONE:]
    packed[...] = pk[...].astype(BF).reshape(32, 16, HX)
    out.wait()


def place(k):
    a, b = k // 3, k % 3
    if b < 2:
        return a * 96, b * C_TWO
    return (288, a * C_TWO) if a < 2 else (384, 0)


def unpack(total, two, one, bias_one, bias_two):
    flat = total[...].astype(F32).reshape(512, HX)
    for k in range(9):
        r, lane = place(k)
        two[3 * k : 3 * k + 3] = flat[r : r + 96, lane : lane + 64].reshape(3, C_ONE, C_TWO)
    for a in range(3):
        for t in range(9):
            r = 384 + a * 40 + t * 4
            one[a * 9 + t] = flat[r : r + 4, 64:96]
    bias_one[...] = flat[384 + 36 : 384 + 37, 64:96]
    bias_two[...] = flat[480:481, 0:64]


def exchange(x, axes):
    return lax.all_to_all(x, axes, 0, 0, tiled=True)


def reduced(x):
    plane = lax.axis_size(PLANE)
    line = lax.axis_size(LINE)
    part = exchange(x, PLANE)
    part = jnp.sum(part, axis=0, dtype=F32).astype(x.dtype)
    part = exchange(jnp.broadcast_to(part[None], (line,) + part.shape), LINE)
    part = jnp.sum(part, axis=0, dtype=F32).astype(x.dtype)
    return exchange(jnp.broadcast_to(part[None], (plane,) + part.shape), PLANE)


def swapped(x, first):
    size = lax.axis_size(DEPTH)
    ups = [(i, i + 1) for i in range(first, size - 1, 2)]
    return lax.ppermute(x, DEPTH, ups + [(j, i) for i, j in ups])


VMEM = pl.BlockSpec(memory_space=pltpu.VMEM)
HBM = pl.BlockSpec(memory_space=pltpu.HBM)
SMEM = pl.BlockSpec(memory_space=pltpu.SMEM)


def local(depth, volumes, w1, b1, w2, b2, cot, interpret=False):
    held = [x if interpret else pltpu.with_memory_space_constraint(x, pltpu.HBM) for x in (w1, b1, w2, b2, cot)]
    ready = pl.pallas_call(
        prepare,
        out_shape=(
            jax.ShapeDtypeStruct((96, 48), BF),
            jax.ShapeDtypeStruct((576, 96), BF),
            jax.ShapeDtypeStruct((288, 192), BF),
            jax.ShapeDtypeStruct((96, HX), F32),
            jax.ShapeDtypeStruct((C_TWO, 2 * CELLS), BF),
        ),
        in_specs=[HBM] * 5,
        out_specs=(VMEM,) * 5,
        scratch_shapes=[
            pltpu.VMEM((27, C_IN, C_ONE), BF),
            pltpu.VMEM((27, C_ONE, C_TWO), BF),
            pltpu.VMEM((1, C_TWO, 2, HY, HX), BF),
            pltpu.VMEM((1, C_ONE), F32),
            pltpu.VMEM((1, C_TWO), F32),
            pltpu.VMEM((144, C_ONE), F32),
            pltpu.VMEM((C_TWO * C_PITCH, HX), F32),
            pltpu.SemaphoreType.DMA((5,)),
        ],
        compiler_params=pltpu.CompilerParams(vmem_limit_bytes=16 * 1024 * 1024),
        interpret=interpret,
        name="prepare",
    )(*held)
    return pl.pallas_call(
        compute,
        out_shape=(
            jax.ShapeDtypeStruct((1, C_TWO, 2, HY, HX), BF),
            jax.ShapeDtypeStruct((32, 16, HX), BF),
        ),
        in_specs=[SMEM] + [VMEM] * 8,
        out_specs=(HBM, VMEM),
        scratch_shapes=[
            pltpu.VMEM((C_IN * V_PITCH, HX), F32),
            pltpu.VMEM((48, 6 * CELLS), F32),
            pltpu.VMEM((48, 6 * CELLS), BF),
            pltpu.VMEM((96, 37 * HX), BF),
            pltpu.VMEM((192, 2 * CELLS), BF),
            pltpu.VMEM((192, 2 * CELLS), BF),
            pltpu.VMEM((C_TWO * C_PITCH, HX), F32),
            pltpu.VMEM((1, C_TWO, 2, HY, HX), BF),
            pltpu.VMEM((C_ONE, 4 * CELLS), F32),
            pltpu.VMEM((288, 2 * CELLS), F32),
            pltpu.VMEM((512, HX), F32),
            pltpu.SemaphoreType.DMA,
        ],
        compiler_params=pltpu.CompilerParams(vmem_limit_bytes=24 * 1024 * 1024),
        interpret=interpret,
        name="slab",
    )(depth, *volumes, *ready)


def split(total, interpret=False):
    return pl.pallas_call(
        unpack,
        out_shape=(
            jax.ShapeDtypeStruct((27, C_ONE, C_TWO), F32),
            jax.ShapeDtypeStruct((27, C_IN, C_ONE), F32),
            jax.ShapeDtypeStruct((1, C_ONE), F32),
            jax.ShapeDtypeStruct((1, C_TWO), F32),
        ),
        in_specs=[VMEM],
        out_specs=(VMEM,) * 4,
        compiler_params=pltpu.CompilerParams(vmem_limit_bytes=4 * 1024 * 1024),
        interpret=interpret,
        name="unpack",
    )(total)


def per_device(volume, kernel_one, bias_one, kernel_two, bias_two, cotangent):
    volumes = (swapped(volume, 0), volume, swapped(volume, 1))
    depth = jnp.stack([lax.axis_index(DEPTH), lax.axis_size(DEPTH)]).astype(jnp.int32)
    w1 = jnp.transpose(kernel_one, (2, 3, 4, 1, 0)).reshape(27, C_IN, C_ONE)
    w2 = jnp.transpose(kernel_two, (2, 3, 4, 1, 0)).reshape(27, C_ONE, C_TWO)
    features, packed = local(depth, volumes, w1, bias_one[None], w2, bias_two[None], cotangent)
    two, one, b1, b2 = split(reduced(packed))
    two = jnp.transpose(two.reshape(3, 3, 3, C_ONE, C_TWO), (4, 3, 0, 1, 2))
    one = jnp.transpose(one.reshape(3, 3, 3, C_IN, C_ONE), (4, 3, 0, 1, 2))
    return (features, one, b1[0], two, b2[0])


def solution(mesh):
    cut = Mesh(mesh.devices.reshape(8, 2, 2, 4, 2), DP + DEPTH)
    return jax.shard_map(
        per_device,
        mesh=cut,
        in_specs=(
            P(DP, None, DEPTH, None, None),
            P(),
            P(),
            P(),
            P(),
            P(DP, None, DEPTH, None, None),
        ),
        out_specs=(P(DP, None, DEPTH, None, None), P(), P(), P(), P()),
        check_vma=False,
    )
```

```python
import jax
import jax.numpy as jnp
from jax import lax
from jax.experimental import pallas as pl
from jax.experimental.pallas import tpu as pltpu
from jax.sharding import Mesh
from jax.sharding import PartitionSpec as P

DP = ("z", "x_hi", "core")
DEPTH = ("y", "x_lo")
PLANE = ("x_hi", "core", "y", "x_lo")
LINE = ("z",)

BF = jnp.bfloat16
F32 = jnp.float32
HY = 8
HX = 128
CELLS = HY * HX
ROWS = HY + 1
C_IN = 4
C_ONE = 32
C_TWO = 64
V_PITCH = 56
C_PITCH = 24


def dot_nn(a, b):
    return lax.dot_general(a, b, (((1,), (0,)), ((), ())), preferred_element_type=F32)


def dot_nt(a, b):
    return lax.dot_general(a, b, (((1,), (1,)), ((), ())), preferred_element_type=F32)


def identity(n):
    return lax.broadcasted_iota(jnp.int32, (n, n), 0) == lax.broadcasted_iota(jnp.int32, (n, n), 1)


def column(row):
    n = row.shape[1]
    return jnp.sum(jnp.where(identity(n), jnp.broadcast_to(row, (n, n)), 0.0), axis=1, keepdims=True)


def transposed(w):
    return dot_nt(identity(w.shape[1]).astype(BF), w).astype(BF)


def sigmoid(v):
    return 1.0 / (1.0 + jnp.exp(-v))


def neighbours(x):
    lane = lax.broadcasted_iota(jnp.int32, x.shape, 1)
    before = jnp.where(lane == 0, 0.0, pltpu.roll(x, 1, 1))
    after = jnp.where(lane == HX - 1, 0.0, pltpu.roll(x, HX - 1, 1))
    return before, x, after


def prepare(w1, b1, w2, b2, c0, w1t, w2t, flip, bias, cot, w1v, w2v, cv, bv1, bv2, w1s, cs, sems):
    copies = [
        pltpu.make_async_copy(src, dst, sems.at[n])
        for n, (src, dst) in enumerate(((w1, w1v), (w2, w2v), (b1, bv1), (b2, bv2), (c0, cv)))
    ]
    for copy in copies:
        copy.start()
    w1s[...] = jnp.zeros((144, C_ONE), F32)
    copies[0].wait()
    for a in range(3):
        for t in range(9):
            w1s[a * 48 + t * 4 : a * 48 + t * 4 + 4, :] = w1v[a * 9 + t].astype(F32)
        w1t[a * C_ONE : (a + 1) * C_ONE, :] = transposed(w1s[a * 48 : (a + 1) * 48, :].astype(BF))
    copies[1].wait()
    for k in range(9):
        w2t[k * C_TWO : (k + 1) * C_TWO, :] = transposed(w2v[3 * k : 3 * k + 3].reshape(96, C_TWO))
        flip[k * C_ONE : (k + 1) * C_ONE, :] = jnp.concatenate([w2v[(8 - k) * 3 + 2 - c] for c in range(3)], axis=1)
    copies[2].wait()
    copies[3].wait()
    bias[0:C_ONE, :] = jnp.broadcast_to(column(bv1[...]), (C_ONE, HX))
    bias[C_ONE:, :] = jnp.broadcast_to(column(bv2[...]), (C_TWO, HX))
    copies[4].wait()
    for o in range(C_TWO):
        for z in range(2):
            cs[o * C_PITCH + z * HY : o * C_PITCH + (z + 1) * HY, :] = cv[0, o, z].astype(F32)
    for row in range(2 * HY):
        cot[:, row * HX : (row + 1) * HX] = cs[pl.ds(row, C_TWO, stride=C_PITCH), :].astype(BF)


def compute(
    depth, va, v0, vb, w1t, w2t, flip, bias, cot,
    features, packed,
    vs, x1, x1b, x3, s3, sb, fs, fb, p1, rs, pk, sem,
):
    even = depth[0] % 2 == 0
    for p in range(6):
        for i in range(C_IN):
            if p in (2, 3):
                plane = v0[0, i, p % 2].astype(F32)
            else:
                near = va[0, i, p % 2].astype(F32)
                far = vb[0, i, p % 2].astype(F32)
                plane = jnp.where(even, far, near) if p < 2 else jnp.where(even, near, far)
            vs[i * V_PITCH + p * HY : i * V_PITCH + (p + 1) * HY, :] = plane
    x1[36:48, :] = jnp.where(lax.broadcasted_iota(jnp.int32, (12, 6 * CELLS), 0) == 0, 1.0, 0.0)
    for p in range(6):
        x1[0:12, p * CELLS : p * CELLS + HX] = jnp.zeros((12, HX), F32)
        x1[24:36, p * CELLS + 7 * HX : (p + 1) * CELLS] = jnp.zeros((12, HX), F32)
        for y in range(HY):
            slab = vs[pl.ds(p * HY + y, C_IN, stride=V_PITCH), :]
            for c, moved in enumerate(neighbours(slab)):
                for b in range(3):
                    to = y + 1 - b
                    if 0 <= to < HY:
                        col = p * CELLS + to * HX
                        x1[b * 12 + c * 4 : b * 12 + c * 4 + 4, col : col + HX] = moved
        x1b[:, p * CELLS : (p + 1) * CELLS] = x1[:, p * CELLS : (p + 1) * CELLS].astype(BF)
    for p in range(5):
        x3[:, p * ROWS * HX : p * ROWS * HX + HX] = jnp.zeros((96, HX), BF)
    for p in range(4):
        pre = bias[0:C_ONE, 0:1]
        for a in range(3):
            pre = pre + dot_nn(w1t[a * C_ONE : (a + 1) * C_ONE, :], x1b[:, (p + a) * CELLS : (p + a + 1) * CELLS])
        sig = sigmoid(pre)
        slope = sig * (1.0 + pre * (1.0 - sig))
        act = pre * sig
        if p in (0, 3):
            inside = jnp.where(depth[0] > 0 if p == 0 else depth[0] < depth[1] - 1, 1.0, 0.0)
            slope = slope * inside
            act = act * inside
        p1[:, p * CELLS : (p + 1) * CELLS] = slope
        for y in range(HY):
            col = (1 + p * ROWS + y) * HX
            for c, moved in enumerate(neighbours(act[:, y * HX : (y + 1) * HX])):
                x3[c * C_ONE : (c + 1) * C_ONE, col : col + HX] = moved.astype(BF)
    for q in range(2):
        sb[0:C_TWO, q * CELLS + 7 * HX : (q + 1) * CELLS] = jnp.zeros((C_TWO, HX), BF)
        sb[2 * C_TWO :, q * CELLS : q * CELLS + HX] = jnp.zeros((C_TWO, HX), BF)
        pre = bias[C_ONE:, 0:1]
        for k in range(9):
            col = ((q + k // 3) * ROWS + k % 3) * HX
            pre = pre + dot_nn(w2t[k * C_TWO : (k + 1) * C_TWO, :], x3[:, col : col + CELLS])
        sig = sigmoid(pre)
        slope = sig * (1.0 + pre * (1.0 - sig))
        act = pre * sig
        for y in range(HY):
            row = q * HY + y
            col = row * HX
            up = cot[:, col : col + HX].astype(F32)
            here = (up * slope[:, y * HX : (y + 1) * HX]).astype(BF)
            for b in range(3):
                to = y + b - 1
                if 0 <= to < HY:
                    sb[b * C_TWO : (b + 1) * C_TWO, q * CELLS + to * HX : q * CELLS + (to + 1) * HX] = here
            for c, moved in enumerate(neighbours(here.astype(F32))):
                s3[c * C_TWO : (c + 1) * C_TWO, col : col + HX] = moved.astype(BF)
            fs[pl.ds(row, C_TWO, stride=C_PITCH), :] = act[:, y * HX : (y + 1) * HX]
    for o in range(C_TWO):
        for z in range(2):
            fb[0, o, z] = fs[o * C_PITCH + z * HY : o * C_PITCH + (z + 1) * HY, :].astype(BF)
    out = pltpu.make_async_copy(fb, features, sem)
    out.start()
    for j in range(2):
        rs[:, j * CELLS : (j + 1) * CELLS] = dot_nn(flip[...], s3[:, j * CELLS : (j + 1) * CELLS])
    pk[384:512, :] = jnp.zeros((128, HX), F32)
    for a in range(3):
        grad = 0.0
        for j in range(2):
            col = (1 + (j + a) * ROWS) * HX
            grad = grad + dot_nt(x3[:, col : col + CELLS], sb[:, j * CELLS : (j + 1) * CELLS])
        for b in range(3):
            row, lane = place(a * 3 + b)
            pk[row : row + 96, lane : lane + C_TWO] = grad[:, b * C_TWO : (b + 1) * C_TWO]
    ones = jnp.ones((8, 2 * CELLS), BF)
    pk[480:488, 0:C_TWO] = dot_nt(ones, s3[C_TWO : 2 * C_TWO, :])
    grads = 0.0
    for t in range(4):
        shares = []
        for y in range(HY):
            back = 0.0
            for k in range(9):
                j, row = t + k // 3 - 2, y + k % 3 - 1
                if 0 <= j < 2 and 0 <= row < HY:
                    col = j * CELLS + row * HX
                    back = back + rs[k * C_ONE : (k + 1) * C_ONE, col : col + HX]
            shares.append(back * p1[:, t * CELLS + y * HX : t * CELLS + (y + 1) * HX])
        share = jnp.concatenate(shares, axis=1)
        high = share.astype(BF)
        share = jnp.concatenate([high, (share - high.astype(F32)).astype(BF)], axis=0)
        near = jnp.concatenate([x1b[:, (t + a) * CELLS : (t + a + 1) * CELLS] for a in range(3)], axis=0)
        grads = grads + dot_nt(near, share)
    for a in range(3):
        grad = grads[a * 48 : a * 48 + 40]
        pk[384 + a * 40 : 384 + a * 40 + 40, C_TWO : C_TWO + C_ONE] = grad[:, :C_ONE] + grad[:, C_ONE:]
    packed[...] = pk[...].astype(BF).reshape(32, 16, HX)
    out.wait()


def place(k):
    a, b = k // 3, k % 3
    if b < 2:
        return a * 96, b * C_TWO
    return (288, a * C_TWO) if a < 2 else (384, 0)


def unpack(total, two, one, bias_one, bias_two):
    flat = total[...].astype(F32).reshape(512, HX)
    for k in range(9):
        r, lane = place(k)
        two[3 * k : 3 * k + 3] = flat[r : r + 96, lane : lane + 64].reshape(3, C_ONE, C_TWO)
    for a in range(3):
        for t in range(9):
            r = 384 + a * 40 + t * 4
            one[a * 9 + t] = flat[r : r + 4, 64:96]
    bias_one[...] = flat[384 + 36 : 384 + 37, 64:96]
    bias_two[...] = flat[480:481, 0:64]


def exchange(x, axes, first):
    order = [first] + [i for i in range(lax.axis_size(axes)) if i != first]
    return lax.all_to_all(x, axes, 0, 0, axis_index_groups=[order], tiled=True)


def middle(axes):
    index = 0
    for axis in axes:
        size = lax.axis_size(axis)
        index = index * size + {"x_hi": 1, "x_lo": 0, "core": 1}.get(axis, size // 2)
    return index


def reduced(x):
    plane = lax.axis_size(PLANE)
    line = lax.axis_size(LINE)
    part = exchange(x, PLANE, middle(PLANE))
    part = jnp.sum(part, axis=0, dtype=F32).astype(x.dtype)
    part = exchange(jnp.broadcast_to(part[None], (line,) + part.shape), LINE, middle(LINE))
    part = jnp.sum(part, axis=0, dtype=F32).astype(x.dtype)
    return exchange(jnp.broadcast_to(part[None], (plane,) + part.shape), PLANE, middle(PLANE))


def swapped(x, first):
    size = lax.axis_size(DEPTH)
    ups = [(i, i + 1) for i in range(first, size - 1, 2)]
    return lax.ppermute(x, DEPTH, ups + [(j, i) for i, j in ups])


VMEM = pl.BlockSpec(memory_space=pltpu.VMEM)
HBM = pl.BlockSpec(memory_space=pltpu.HBM)
SMEM = pl.BlockSpec(memory_space=pltpu.SMEM)


def local(depth, volumes, w1, b1, w2, b2, cot, interpret=False):
    held = [x if interpret else pltpu.with_memory_space_constraint(x, pltpu.HBM) for x in (w1, b1, w2, b2, cot)]
    ready = pl.pallas_call(
        prepare,
        out_shape=(
            jax.ShapeDtypeStruct((96, 48), BF),
            jax.ShapeDtypeStruct((576, 96), BF),
            jax.ShapeDtypeStruct((288, 192), BF),
            jax.ShapeDtypeStruct((96, HX), F32),
            jax.ShapeDtypeStruct((C_TWO, 2 * CELLS), BF),
        ),
        in_specs=[HBM] * 5,
        out_specs=(VMEM,) * 5,
        scratch_shapes=[
            pltpu.VMEM((27, C_IN, C_ONE), BF),
            pltpu.VMEM((27, C_ONE, C_TWO), BF),
            pltpu.VMEM((1, C_TWO, 2, HY, HX), BF),
            pltpu.VMEM((1, C_ONE), F32),
            pltpu.VMEM((1, C_TWO), F32),
            pltpu.VMEM((144, C_ONE), F32),
            pltpu.VMEM((C_TWO * C_PITCH, HX), F32),
            pltpu.SemaphoreType.DMA((5,)),
        ],
        compiler_params=pltpu.CompilerParams(vmem_limit_bytes=16 * 1024 * 1024),
        interpret=interpret,
        name="prepare",
    )(*held)
    return pl.pallas_call(
        compute,
        out_shape=(
            jax.ShapeDtypeStruct((1, C_TWO, 2, HY, HX), BF),
            jax.ShapeDtypeStruct((32, 16, HX), BF),
        ),
        in_specs=[SMEM] + [VMEM] * 8,
        out_specs=(HBM, VMEM),
        scratch_shapes=[
            pltpu.VMEM((C_IN * V_PITCH, HX), F32),
            pltpu.VMEM((48, 6 * CELLS), F32),
            pltpu.VMEM((48, 6 * CELLS), BF),
            pltpu.VMEM((96, 37 * HX), BF),
            pltpu.VMEM((192, 2 * CELLS), BF),
            pltpu.VMEM((192, 2 * CELLS), BF),
            pltpu.VMEM((C_TWO * C_PITCH, HX), F32),
            pltpu.VMEM((1, C_TWO, 2, HY, HX), BF),
            pltpu.VMEM((C_ONE, 4 * CELLS), F32),
            pltpu.VMEM((288, 2 * CELLS), F32),
            pltpu.VMEM((512, HX), F32),
            pltpu.SemaphoreType.DMA,
        ],
        compiler_params=pltpu.CompilerParams(vmem_limit_bytes=24 * 1024 * 1024),
        interpret=interpret,
        name="slab",
    )(depth, *volumes, *ready)


def split(total, interpret=False):
    return pl.pallas_call(
        unpack,
        out_shape=(
            jax.ShapeDtypeStruct((27, C_ONE, C_TWO), F32),
            jax.ShapeDtypeStruct((27, C_IN, C_ONE), F32),
            jax.ShapeDtypeStruct((1, C_ONE), F32),
            jax.ShapeDtypeStruct((1, C_TWO), F32),
        ),
        in_specs=[VMEM],
        out_specs=(VMEM,) * 4,
        compiler_params=pltpu.CompilerParams(vmem_limit_bytes=4 * 1024 * 1024),
        interpret=interpret,
        name="unpack",
    )(total)


def per_device(volume, kernel_one, bias_one, kernel_two, bias_two, cotangent):
    volumes = (swapped(volume, 0), volume, swapped(volume, 1))
    depth = jnp.stack([lax.axis_index(DEPTH), lax.axis_size(DEPTH)]).astype(jnp.int32)
    w1 = jnp.transpose(kernel_one, (2, 3, 4, 1, 0)).reshape(27, C_IN, C_ONE)
    w2 = jnp.transpose(kernel_two, (2, 3, 4, 1, 0)).reshape(27, C_ONE, C_TWO)
    features, packed = local(depth, volumes, w1, bias_one[None], w2, bias_two[None], cotangent)
    two, one, b1, b2 = split(reduced(packed))
    two = jnp.transpose(two.reshape(3, 3, 3, C_ONE, C_TWO), (4, 3, 0, 1, 2))
    one = jnp.transpose(one.reshape(3, 3, 3, C_IN, C_ONE), (4, 3, 0, 1, 2))
    return (features, one, b1[0], two, b2[0])


def solution(mesh):
    cut = Mesh(mesh.devices.reshape(8, 2, 2, 4, 2), DP + DEPTH)
    return jax.shard_map(
        per_device,
        mesh=cut,
        in_specs=(
            P(DP, None, DEPTH, None, None),
            P(),
            P(),
            P(),
            P(),
            P(DP, None, DEPTH, None, None),
        ),
        out_specs=(P(DP, None, DEPTH, None, None), P(), P(), P(), P()),
        check_vma=False,
    )
```

```python
import jax
import jax.numpy as jnp
from jax import lax
from jax.experimental import pallas as pl
from jax.experimental.pallas import tpu as pltpu
from jax.sharding import Mesh
from jax.sharding import PartitionSpec as P

DP = ("z", "x_hi", "core")
DEPTH = ("y", "x_lo")
PLANE = ("x_hi", "core", "y", "x_lo")
LINE = ("z",)

BF = jnp.bfloat16
F32 = jnp.float32
HY = 8
HX = 128
CELLS = HY * HX
ROWS = HY + 1
C_IN = 4
C_ONE = 32
C_TWO = 64
STEP = 8
V_PITCH = 56
C_PITCH = 24


def dot_nn(a, b):
    return lax.dot_general(a, b, (((1,), (0,)), ((), ())), preferred_element_type=F32)


def dot_nt(a, b):
    return lax.dot_general(a, b, (((1,), (1,)), ((), ())), preferred_element_type=F32)


def identity(n):
    return lax.broadcasted_iota(jnp.int32, (n, n), 0) == lax.broadcasted_iota(jnp.int32, (n, n), 1)


def column(row):
    n = row.shape[1]
    return jnp.sum(jnp.where(identity(n), jnp.broadcast_to(row, (n, n)), 0.0), axis=1, keepdims=True)


def transposed(w):
    return dot_nt(identity(w.shape[1]).astype(BF), w).astype(BF)


def sigmoid(v):
    return 1.0 / (1.0 + jnp.exp(-v))


def neighbours(x):
    lane = lax.broadcasted_iota(jnp.int32, x.shape, 1)
    before = jnp.where(lane == 0, 0.0, pltpu.roll(x, 1, 1))
    after = jnp.where(lane == HX - 1, 0.0, pltpu.roll(x, HX - 1, 1))
    return before, x, after


def prepare(w1, b1, w2, b2, c0, w1t, w2t, flip, bias, cot, w1v, w2v, cv, bv1, bv2, w1s, cs, sems):
    copies = [
        pltpu.make_async_copy(src, dst, sems.at[n])
        for n, (src, dst) in enumerate(((w1, w1v), (w2, w2v), (b1, bv1), (b2, bv2), (c0, cv)))
    ]
    for copy in copies:
        copy.start()
    w1s[...] = jnp.zeros((144, C_ONE), F32)
    copies[0].wait()
    for a in range(3):
        for t in range(9):
            row = a * 48 + t // 3 * 16 + t % 3 * 4
            w1s[row : row + 4, :] = w1v[a * 9 + t].astype(F32)
    w1t[...] = transposed(w1s[...].astype(BF))
    copies[1].wait()
    w2t[...] = transposed(w2v[...].reshape(864, C_TWO))
    for k in range(9):
        flip[k * C_ONE : (k + 1) * C_ONE, :] = jnp.concatenate([w2v[(8 - k) * 3 + 2 - c] for c in range(3)], axis=1)
    copies[2].wait()
    copies[3].wait()
    bias[0:C_ONE, :] = jnp.broadcast_to(column(bv1[...]), (C_ONE, HX))
    bias[C_ONE:, :] = jnp.broadcast_to(column(bv2[...]), (C_TWO, HX))
    copies[4].wait()
    for o in range(C_TWO):
        for z in range(2):
            cs[o * C_PITCH + z * HY : o * C_PITCH + (z + 1) * HY, :] = cv[0, o, z].astype(F32)
    for row in range(2 * HY):
        cot[:, row * HX : (row + 1) * HX] = cs[pl.ds(row, C_TWO, stride=C_PITCH), :].astype(BF)


def compute(
    depth, va, v0, vb, w1t, w2t, flip, bias, cot,
    features, packed,
    vs, x1b, x3, s3, sb, fs, fb, p1, rs, pk, sem,
):
    even = depth[0] % 2 == 0
    for p in range(6):
        for i in range(C_IN):
            if p in (2, 3):
                plane = v0[0, i, p % 2].astype(F32)
            else:
                near = va[0, i, p % 2].astype(F32)
                far = vb[0, i, p % 2].astype(F32)
                plane = jnp.where(even, far, near) if p < 2 else jnp.where(even, near, far)
            vs[i * V_PITCH + p * HY : i * V_PITCH + (p + 1) * HY, :] = plane
    last = jnp.where(lax.broadcasted_iota(jnp.int32, (4, HX), 0) == 0, 1.0, 0.0)
    edge = jnp.concatenate([jnp.zeros((12, HX), F32), last], axis=0).astype(BF)
    for p in range(6):
        x1b[0:16, p * CELLS : p * CELLS + HX] = edge
        x1b[32:48, p * CELLS + 7 * HX : (p + 1) * CELLS] = edge
        for y in range(HY):
            before, slab, after = neighbours(vs[pl.ds(p * HY + y, C_IN, stride=V_PITCH), :])
            moved = jnp.concatenate([before, slab, after, last], axis=0).astype(BF)
            for b in range(3):
                to = y + 1 - b
                if 0 <= to < HY:
                    x1b[b * 16 : b * 16 + 16, p * CELLS + to * HX : p * CELLS + (to + 1) * HX] = moved
    for p in range(5):
        x3[:, p * ROWS * HX : p * ROWS * HX + HX] = jnp.zeros((96, HX), BF)
    pk[384:512, :] = jnp.zeros((128, HX), F32)

    def planes(p):
        return jnp.concatenate([x1b[:, (p + a) * CELLS : (p + a + 1) * CELLS] for a in range(3)], axis=0)

    def first(p):
        pre = dot_nn(w1t[...], planes(p)) + bias[0:C_ONE, 0:1]
        sig = sigmoid(pre)
        slope = sig * (1.0 + pre * (1.0 - sig))
        act = pre * sig
        if p in (0, 3):
            inside = jnp.where(depth[0] > 0 if p == 0 else depth[0] < depth[1] - 1, 1.0, 0.0)
            slope = slope * inside
            act = act * inside
        p1[:, p * CELLS : (p + 1) * CELLS] = slope
        for y in range(HY):
            col = (1 + p * ROWS + y) * HX
            for c, moved in enumerate(neighbours(act[:, y * HX : (y + 1) * HX])):
                x3[c * C_ONE : (c + 1) * C_ONE, col : col + HX] = moved.astype(BF)

    def second(q):
        sb[0:C_TWO, q * CELLS + 7 * HX : (q + 1) * CELLS] = jnp.zeros((C_TWO, HX), BF)
        sb[2 * C_TWO :, q * CELLS : q * CELLS + HX] = jnp.zeros((C_TWO, HX), BF)
        for part in range(0, HY, STEP):
            cols = [((q + k // 3) * ROWS + k % 3 + part) * HX for k in range(9)]
            near = jnp.concatenate([x3[:, col : col + STEP * HX] for col in cols], axis=0)
            pre = dot_nn(w2t[...], near) + bias[C_ONE:, 0:1]
            sig = sigmoid(pre)
            slope = sig * (1.0 + pre * (1.0 - sig))
            act = pre * sig
            for y in range(part, part + STEP):
                row = q * HY + y
                col = row * HX
                lane = (y - part) * HX
                up = cot[:, col : col + HX].astype(F32)
                here = (up * slope[:, lane : lane + HX]).astype(BF)
                for b in range(3):
                    to = y + b - 1
                    if 0 <= to < HY:
                        sb[b * C_TWO : (b + 1) * C_TWO, q * CELLS + to * HX : q * CELLS + (to + 1) * HX] = here
                for c, moved in enumerate(neighbours(here.astype(F32))):
                    s3[c * C_TWO : (c + 1) * C_TWO, col : col + HX] = moved.astype(BF)
                fs[pl.ds(row, C_TWO, stride=C_PITCH), :] = act[:, lane : lane + HX]
        for o in range(C_TWO):
            fb[0, o, q] = fs[o * C_PITCH + q * HY : o * C_PITCH + (q + 1) * HY, :].astype(BF)

    def back(j):
        rs[:, j * CELLS : (j + 1) * CELLS] = dot_nn(flip[...], s3[:, j * CELLS : (j + 1) * CELLS])

    def two(j):
        near = [x3[:, (1 + (j + a) * ROWS) * HX : (1 + (j + a) * ROWS) * HX + CELLS] for a in range(3)]
        near = jnp.concatenate(near + [jnp.ones((16, CELLS), BF)], axis=0)
        return dot_nt(near, sb[:, j * CELLS : (j + 1) * CELLS])

    first(0)
    first(1)
    first(2)
    first(3)
    second(0)
    second(1)
    back(0)
    back(1)
    two_0 = two(0)
    two_1 = two(1)
    out = pltpu.make_async_copy(fb, features, sem)
    out.start()
    twos = two_0 + two_1
    for k in range(9):
        row, lane = place(k)
        pk[row : row + 96, lane : lane + C_TWO] = twos[k // 3 * 96 : k // 3 * 96 + 96, k % 3 * C_TWO : k % 3 * C_TWO + C_TWO]
    pk[480:488, C_TWO : 2 * C_TWO] = twos[288:296, C_TWO : 2 * C_TWO]
    grads = 0.0
    for t in range(4):
        shares = []
        for y in range(HY):
            total = 0.0
            for k in range(9):
                j, row = t + k // 3 - 2, y + k % 3 - 1
                if 0 <= j < 2 and 0 <= row < HY:
                    col = j * CELLS + row * HX
                    total = total + rs[k * C_ONE : (k + 1) * C_ONE, col : col + HX]
            shares.append(total * p1[:, t * CELLS + y * HX : t * CELLS + (y + 1) * HX])
        share = jnp.concatenate(shares, axis=1)
        high = share.astype(BF)
        share = jnp.concatenate([high, (share - high.astype(F32)).astype(BF)], axis=0)
        grads = grads + dot_nt(planes(t), share)
    grads = grads[:, :C_ONE] + grads[:, C_ONE:]
    for a in range(3):
        row, lane = place_one(a)
        pk[row : row + 48, lane : lane + C_ONE] = grads[a * 48 : a * 48 + 48]
    packed[...] = pk[...].astype(BF).reshape(32, 16, HX)
    out.wait()


def place(k):
    a, b = k // 3, k % 3
    if b < 2:
        return a * 96, b * C_TWO
    return (288, a * C_TWO) if a < 2 else (384, 0)


def place_one(a):
    return 384 + a % 2 * 48, C_TWO + a // 2 * C_ONE


def unpack(total, two, one, bias_one, bias_two):
    flat = total[...].astype(F32).reshape(512, HX)
    for k in range(9):
        r, lane = place(k)
        two[3 * k : 3 * k + 3] = flat[r : r + 96, lane : lane + 64].reshape(3, C_ONE, C_TWO)
    for a in range(3):
        r, lane = place_one(a)
        for t in range(9):
            row = r + t // 3 * 16 + t % 3 * 4
            one[a * 9 + t] = flat[row : row + 4, lane : lane + C_ONE]
    bias_one[...] = flat[384 + 12 : 384 + 13, C_TWO : C_TWO + C_ONE]
    bias_two[...] = flat[480:481, C_TWO : 2 * C_TWO]


def exchange(x, axes, first):
    order = [first] + [i for i in range(lax.axis_size(axes)) if i != first]
    return lax.all_to_all(x, axes, 0, 0, axis_index_groups=[order], tiled=True)


def middle(axes):
    index = 0
    for axis in axes:
        size = lax.axis_size(axis)
        index = index * size + {"x_hi": 1, "x_lo": 0, "core": 1}.get(axis, size // 2)
    return index


def reduced(x):
    plane = lax.axis_size(PLANE)
    line = lax.axis_size(LINE)
    part = exchange(x, PLANE, middle(PLANE))
    part = jnp.sum(part, axis=0, dtype=F32).astype(x.dtype)
    part = exchange(jnp.broadcast_to(part[None], (line,) + part.shape), LINE, middle(LINE))
    part = jnp.sum(part, axis=0, dtype=F32).astype(x.dtype)
    return exchange(jnp.broadcast_to(part[None], (plane,) + part.shape), PLANE, middle(PLANE))


def swapped(x, first):
    size = lax.axis_size(DEPTH)
    ups = [(i, i + 1) for i in range(first, size - 1, 2)]
    return lax.ppermute(x, DEPTH, ups + [(j, i) for i, j in ups])


VMEM = pl.BlockSpec(memory_space=pltpu.VMEM)
HBM = pl.BlockSpec(memory_space=pltpu.HBM)
SMEM = pl.BlockSpec(memory_space=pltpu.SMEM)


def local(depth, volumes, w1, b1, w2, b2, cot, interpret=False):
    held = [x if interpret else pltpu.with_memory_space_constraint(x, pltpu.HBM) for x in (w1, b1, w2, b2, cot)]
    ready = pl.pallas_call(
        prepare,
        out_shape=(
            jax.ShapeDtypeStruct((C_ONE, 144), BF),
            jax.ShapeDtypeStruct((C_TWO, 864), BF),
            jax.ShapeDtypeStruct((288, 192), BF),
            jax.ShapeDtypeStruct((96, HX), F32),
            jax.ShapeDtypeStruct((C_TWO, 2 * CELLS), BF),
        ),
        in_specs=[HBM] * 5,
        out_specs=(VMEM,) * 5,
        scratch_shapes=[
            pltpu.VMEM((27, C_IN, C_ONE), BF),
            pltpu.VMEM((27, C_ONE, C_TWO), BF),
            pltpu.VMEM((1, C_TWO, 2, HY, HX), BF),
            pltpu.VMEM((1, C_ONE), F32),
            pltpu.VMEM((1, C_TWO), F32),
            pltpu.VMEM((144, C_ONE), F32),
            pltpu.VMEM((C_TWO * C_PITCH, HX), F32),
            pltpu.SemaphoreType.DMA((5,)),
        ],
        compiler_params=pltpu.CompilerParams(vmem_limit_bytes=16 * 1024 * 1024),
        interpret=interpret,
        name="prepare",
    )(*held)
    return pl.pallas_call(
        compute,
        out_shape=(
            jax.ShapeDtypeStruct((1, C_TWO, 2, HY, HX), BF),
            jax.ShapeDtypeStruct((32, 16, HX), BF),
        ),
        in_specs=[SMEM] + [VMEM] * 8,
        out_specs=(HBM, VMEM),
        scratch_shapes=[
            pltpu.VMEM((C_IN * V_PITCH, HX), F32),
            pltpu.VMEM((48, 6 * CELLS), BF),
            pltpu.VMEM((96, 37 * HX), BF),
            pltpu.VMEM((192, 2 * CELLS), BF),
            pltpu.VMEM((192, 2 * CELLS), BF),
            pltpu.VMEM((C_TWO * C_PITCH, HX), F32),
            pltpu.VMEM((1, C_TWO, 2, HY, HX), BF),
            pltpu.VMEM((C_ONE, 4 * CELLS), F32),
            pltpu.VMEM((288, 2 * CELLS), F32),
            pltpu.VMEM((512, HX), F32),
            pltpu.SemaphoreType.DMA,
        ],
        compiler_params=pltpu.CompilerParams(vmem_limit_bytes=24 * 1024 * 1024),
        interpret=interpret,
        name="slab",
    )(depth, *volumes, *ready)


def split(total, interpret=False):
    return pl.pallas_call(
        unpack,
        out_shape=(
            jax.ShapeDtypeStruct((27, C_ONE, C_TWO), F32),
            jax.ShapeDtypeStruct((27, C_IN, C_ONE), F32),
            jax.ShapeDtypeStruct((1, C_ONE), F32),
            jax.ShapeDtypeStruct((1, C_TWO), F32),
        ),
        in_specs=[VMEM],
        out_specs=(VMEM,) * 4,
        compiler_params=pltpu.CompilerParams(vmem_limit_bytes=4 * 1024 * 1024),
        interpret=interpret,
        name="unpack",
    )(total)


def per_device(volume, kernel_one, bias_one, kernel_two, bias_two, cotangent):
    volumes = (swapped(volume, 0), volume, swapped(volume, 1))
    depth = jnp.stack([lax.axis_index(DEPTH), lax.axis_size(DEPTH)]).astype(jnp.int32)
    w1 = jnp.transpose(kernel_one, (2, 3, 4, 1, 0)).reshape(27, C_IN, C_ONE)
    w2 = jnp.transpose(kernel_two, (2, 3, 4, 1, 0)).reshape(27, C_ONE, C_TWO)
    features, packed = local(depth, volumes, w1, bias_one[None], w2, bias_two[None], cotangent)
    two, one, b1, b2 = split(reduced(packed))
    two = jnp.transpose(two.reshape(3, 3, 3, C_ONE, C_TWO), (4, 3, 0, 1, 2))
    one = jnp.transpose(one.reshape(3, 3, 3, C_IN, C_ONE), (4, 3, 0, 1, 2))
    return (features, one, b1[0], two, b2[0])


def solution(mesh):
    cut = Mesh(mesh.devices.reshape(8, 2, 2, 4, 2), DP + DEPTH)
    return jax.shard_map(
        per_device,
        mesh=cut,
        in_specs=(
            P(DP, None, DEPTH, None, None),
            P(),
            P(),
            P(),
            P(),
            P(DP, None, DEPTH, None, None),
        ),
        out_specs=(P(DP, None, DEPTH, None, None), P(), P(), P(), P()),
        check_vma=False,
    )
```

```python
import jax
import jax.numpy as jnp
from jax import lax
from jax.experimental import pallas as pl
from jax.experimental.pallas import tpu as pltpu
from jax.sharding import Mesh
from jax.sharding import PartitionSpec as P

DP = ("z", "x_hi", "core")
DEPTH = ("y", "x_lo")
PLANE = ("x_hi", "core", "y", "x_lo")
LINE = ("z",)

BF = jnp.bfloat16
F32 = jnp.float32
HY = 8
HX = 128
CELLS = HY * HX
ROWS = HY + 1
C_IN = 4
C_ONE = 32
C_TWO = 64
STEP = 8
V_PITCH = 56
C_PITCH = 24


def dot_nn(a, b):
    return lax.dot_general(a, b, (((1,), (0,)), ((), ())), preferred_element_type=F32)


def dot_nt(a, b):
    return lax.dot_general(a, b, (((1,), (1,)), ((), ())), preferred_element_type=F32)


def identity(n):
    return lax.broadcasted_iota(jnp.int32, (n, n), 0) == lax.broadcasted_iota(jnp.int32, (n, n), 1)


def column(row):
    n = row.shape[1]
    return jnp.sum(jnp.where(identity(n), jnp.broadcast_to(row, (n, n)), 0.0), axis=1, keepdims=True)


def transposed(w):
    return dot_nt(identity(w.shape[1]).astype(BF), w).astype(BF)


def sigmoid(v):
    return 1.0 / (1.0 + jnp.exp(-v))


def neighbours(x):
    lane = lax.broadcasted_iota(jnp.int32, x.shape, 1)
    zero = jnp.zeros((), x.dtype)
    before = jnp.where(lane == 0, zero, pltpu.roll(x, 1, 1))
    after = jnp.where(lane == HX - 1, zero, pltpu.roll(x, HX - 1, 1))
    return before, x, after


def taps(to, p, load):
    last = jnp.where(lax.broadcasted_iota(jnp.int32, (4, HX), 0) == 0, 1.0, 0.0)
    edge = jnp.concatenate([jnp.zeros((12, HX), F32), last], axis=0).astype(BF)
    to[0:16, p * CELLS : p * CELLS + HX] = edge
    to[32:48, p * CELLS + 7 * HX : (p + 1) * CELLS] = edge
    for y in range(HY):
        before, slab, after = neighbours(load(y))
        moved = jnp.concatenate([before, slab, after, last], axis=0).astype(BF)
        for b in range(3):
            row = y + 1 - b
            if 0 <= row < HY:
                to[b * 16 : b * 16 + 16, p * CELLS + row * HX : p * CELLS + (row + 1) * HX] = moved


def prepare(
    v0, w1, b1, w2, b2, c0,
    own, w1t, w2t, flip, bias, cot,
    vv, w1v, w2v, cv, bv1, bv2, vs, w1s, cs, sems,
):
    copies = [
        pltpu.make_async_copy(src, dst, sems.at[n])
        for n, (src, dst) in enumerate(((w1, w1v), (w2, w2v), (b1, bv1), (b2, bv2), (c0, cv), (v0, vv)))
    ]
    for copy in copies:
        copy.start()
    w1s[...] = jnp.zeros((144, C_ONE), F32)
    copies[0].wait()
    for a in range(3):
        for t in range(9):
            row = a * 48 + t // 3 * 16 + t % 3 * 4
            w1s[row : row + 4, :] = w1v[a * 9 + t].astype(F32)
    w1t[...] = transposed(w1s[...].astype(BF))
    copies[1].wait()
    w2t[...] = transposed(w2v[...].reshape(864, C_TWO))
    for k in range(9):
        flip[k * C_ONE : (k + 1) * C_ONE, :] = jnp.concatenate([w2v[(8 - k) * 3 + 2 - c] for c in range(3)], axis=1)
    copies[2].wait()
    copies[3].wait()
    bias[0:C_ONE, :] = jnp.broadcast_to(column(bv1[...]), (C_ONE, HX))
    bias[C_ONE:, :] = jnp.broadcast_to(column(bv2[...]), (C_TWO, HX))
    copies[5].wait()
    for p in range(2):
        for i in range(C_IN):
            vs[i * V_PITCH + p * HY : i * V_PITCH + (p + 1) * HY, :] = vv[0, i, p].astype(F32)
    for p in range(2):
        taps(own, p, lambda y: vs[pl.ds(p * HY + y, C_IN, stride=V_PITCH), :])
    copies[4].wait()
    for o in range(C_TWO):
        for z in range(2):
            cs[o * C_PITCH + z * HY : o * C_PITCH + (z + 1) * HY, :] = cv[0, o, z].astype(F32)
    for row in range(2 * HY):
        cot[:, row * HX : (row + 1) * HX] = cs[pl.ds(row, C_TWO, stride=C_PITCH), :].astype(BF)


def compute(
    depth, va, vb, own, w1t, w2t, flip, bias, cot,
    features, packed,
    vs, x1b, x3, s3, sb, fs, fb, p1, rs, sem,
):
    even = depth[0] % 2 == 1
    for p in range(4):
        for i in range(C_IN):
            near = va[0, i, p % 2].astype(F32)
            far = vb[0, i, p % 2].astype(F32)
            plane = jnp.where(even, far, near) if p < 2 else jnp.where(even, near, far)
            vs[i * V_PITCH + p * HY : i * V_PITCH + (p + 1) * HY, :] = plane
    for p in range(4):
        taps(x1b, p, lambda y: vs[pl.ds(p * HY + y, C_IN, stride=V_PITCH), :])
    for p in range(5):
        x3[:, p * ROWS * HX : p * ROWS * HX + HX] = jnp.zeros((96, HX), BF)

    def planes(p):
        parts = []
        for q in (p, p + 1, p + 2):
            ref, at = (own, q - 2) if q in (2, 3) else (x1b, q if q < 2 else q - 2)
            parts.append(ref[:, at * CELLS : (at + 1) * CELLS])
        return jnp.concatenate(parts, axis=0)

    def first(p):
        pre = dot_nn(w1t[...], planes(p)) + bias[0:C_ONE, 0:1]
        sig = sigmoid(pre)
        act = pre * sig
        slope = sig + act * (1.0 - sig)
        if p in (0, 3):
            inside = jnp.where(depth[0] > 0 if p == 0 else depth[0] < depth[1] - 1, 1.0, 0.0)
            slope = slope * inside
            act = act * inside
        p1[:, p * CELLS : (p + 1) * CELLS] = slope
        for y in range(HY):
            col = (1 + p * ROWS + y) * HX
            for c, moved in enumerate(neighbours(act[:, y * HX : (y + 1) * HX].astype(BF))):
                x3[c * C_ONE : (c + 1) * C_ONE, col : col + HX] = moved

    def second(q):
        sb[0:C_TWO, q * CELLS + 7 * HX : (q + 1) * CELLS] = jnp.zeros((C_TWO, HX), BF)
        sb[2 * C_TWO :, q * CELLS : q * CELLS + HX] = jnp.zeros((C_TWO, HX), BF)
        for part in range(0, HY, STEP):
            cols = [((q + k // 3) * ROWS + k % 3 + part) * HX for k in range(9)]
            near = jnp.concatenate([x3[:, col : col + STEP * HX] for col in cols], axis=0)
            pre = dot_nn(w2t[...], near) + bias[C_ONE:, 0:1]
            sig = sigmoid(pre)
            act = pre * sig
            slope = sig + act * (1.0 - sig)
            for y in range(part, part + STEP):
                row = q * HY + y
                col = row * HX
                lane = (y - part) * HX
                up = cot[:, col : col + HX].astype(F32)
                here = (up * slope[:, lane : lane + HX]).astype(BF)
                for b in range(3):
                    to = y + b - 1
                    if 0 <= to < HY:
                        sb[b * C_TWO : (b + 1) * C_TWO, q * CELLS + to * HX : q * CELLS + (to + 1) * HX] = here
                for c, moved in enumerate(neighbours(here)):
                    s3[c * C_TWO : (c + 1) * C_TWO, col : col + HX] = moved
                fs[pl.ds(row, C_TWO, stride=C_PITCH), :] = act[:, lane : lane + HX]
        for o in range(C_TWO):
            fb[0, o, q] = fs[o * C_PITCH + q * HY : o * C_PITCH + (q + 1) * HY, :].astype(BF)

    def back(j):
        rs[:, j * CELLS : (j + 1) * CELLS] = dot_nn(flip[...], s3[:, j * CELLS : (j + 1) * CELLS])

    def two(j):
        near = [x3[:, (1 + (j + a) * ROWS) * HX : (1 + (j + a) * ROWS) * HX + CELLS] for a in range(3)]
        near = jnp.concatenate(near + [jnp.ones((16, CELLS), BF)], axis=0)
        return dot_nt(near, sb[:, j * CELLS : (j + 1) * CELLS])

    first(0)
    first(1)
    first(2)
    first(3)
    second(0)
    second(1)
    back(0)
    back(1)
    two_0 = two(0)
    two_1 = two(1)
    out = pltpu.make_async_copy(fb, features, sem)
    out.start()
    twos = two_0 + two_1
    grads = 0.0
    for t in range(4):
        shares = []
        for y in range(HY):
            total = 0.0
            for k in range(9):
                j, row = t + k // 3 - 2, y + k % 3 - 1
                if 0 <= j < 2 and 0 <= row < HY:
                    col = j * CELLS + row * HX
                    total = total + rs[k * C_ONE : (k + 1) * C_ONE, col : col + HX]
            shares.append(total * p1[:, t * CELLS + y * HX : t * CELLS + (y + 1) * HX])
        share = jnp.concatenate(shares, axis=1)
        high = share.astype(BF)
        share = jnp.concatenate([high, (share - high.astype(F32)).astype(BF)], axis=0)
        grads = grads + dot_nt(planes(t), share)
    grads = grads[:, :C_ONE] + grads[:, C_ONE:]
    side = twos[:, 2 * C_TWO :]
    third = jnp.concatenate([grads[96:], jnp.zeros((48, C_ONE), F32)], axis=0)
    rows = jnp.concatenate(
        [
            twos[:288, : 2 * C_TWO],
            jnp.concatenate([side[:96], side[96:192]], axis=1),
            jnp.concatenate([side[192:288], grads[:96], third], axis=1),
            twos[288:, : 2 * C_TWO],
            jnp.zeros((16, HX), F32),
        ],
        axis=0,
    )
    packed[...] = rows.astype(BF).reshape(32, 16, HX)
    out.wait()


def place(k):
    a, b = k // 3, k % 3
    if b < 2:
        return a * 96, b * C_TWO
    return (288, a * C_TWO) if a < 2 else (384, 0)


def place_one(a):
    return 384 + a % 2 * 48, C_TWO + a // 2 * C_ONE


def unpack(total, two, one, bias_one, bias_two):
    flat = total[...].astype(F32).reshape(512, HX)
    for k in range(9):
        r, lane = place(k)
        two[3 * k : 3 * k + 3] = flat[r : r + 96, lane : lane + 64].reshape(3, C_ONE, C_TWO)
    for a in range(3):
        r, lane = place_one(a)
        for t in range(9):
            row = r + t // 3 * 16 + t % 3 * 4
            one[a * 9 + t] = flat[row : row + 4, lane : lane + C_ONE]
    bias_one[...] = flat[384 + 12 : 384 + 13, C_TWO : C_TWO + C_ONE]
    bias_two[...] = flat[480:481, C_TWO : 2 * C_TWO]


def exchange(x, axes, first):
    order = [first] + [i for i in range(lax.axis_size(axes)) if i != first]
    return lax.all_to_all(x, axes, 0, 0, axis_index_groups=[order], tiled=True)


def middle(axes):
    index = 0
    for axis in axes:
        size = lax.axis_size(axis)
        index = index * size + {"x_hi": 1, "x_lo": 0, "core": 1}.get(axis, size // 2)
    return index


def reduced(x):
    plane = lax.axis_size(PLANE)
    line = lax.axis_size(LINE)
    part = exchange(x, PLANE, middle(PLANE))
    part = jnp.sum(part, axis=0, dtype=F32).astype(x.dtype)
    part = exchange(jnp.broadcast_to(part[None], (line,) + part.shape), LINE, middle(LINE))
    part = jnp.sum(part, axis=0, dtype=F32).astype(x.dtype)
    return exchange(jnp.broadcast_to(part[None], (plane,) + part.shape), PLANE, middle(PLANE))


def swapped(x, first):
    size = lax.axis_size(DEPTH)
    ups = [(i, i + 1) for i in range(first, size - 1, 2)]
    return lax.ppermute(x, DEPTH, ups + [(j, i) for i, j in ups])


VMEM = pl.BlockSpec(memory_space=pltpu.VMEM)
HBM = pl.BlockSpec(memory_space=pltpu.HBM)
SMEM = pl.BlockSpec(memory_space=pltpu.SMEM)


def local(depth, va, v0, vb, w1, b1, w2, b2, cot, interpret=False):
    held = [x if interpret else pltpu.with_memory_space_constraint(x, pltpu.HBM) for x in (v0, w1, b1, w2, b2, cot)]
    ready = pl.pallas_call(
        prepare,
        out_shape=(
            jax.ShapeDtypeStruct((48, 2 * CELLS), BF),
            jax.ShapeDtypeStruct((C_ONE, 144), BF),
            jax.ShapeDtypeStruct((C_TWO, 864), BF),
            jax.ShapeDtypeStruct((288, 192), BF),
            jax.ShapeDtypeStruct((96, HX), F32),
            jax.ShapeDtypeStruct((C_TWO, 2 * CELLS), BF),
        ),
        in_specs=[HBM] * 6,
        out_specs=(VMEM,) * 6,
        scratch_shapes=[
            pltpu.VMEM((1, C_IN, 2, HY, HX), BF),
            pltpu.VMEM((27, C_IN, C_ONE), BF),
            pltpu.VMEM((27, C_ONE, C_TWO), BF),
            pltpu.VMEM((1, C_TWO, 2, HY, HX), BF),
            pltpu.VMEM((1, C_ONE), F32),
            pltpu.VMEM((1, C_TWO), F32),
            pltpu.VMEM((C_IN * V_PITCH, HX), F32),
            pltpu.VMEM((144, C_ONE), F32),
            pltpu.VMEM((C_TWO * C_PITCH, HX), F32),
            pltpu.SemaphoreType.DMA((6,)),
        ],
        compiler_params=pltpu.CompilerParams(vmem_limit_bytes=16 * 1024 * 1024),
        interpret=interpret,
        name="prepare",
    )(*held)
    return pl.pallas_call(
        compute,
        out_shape=(
            jax.ShapeDtypeStruct((1, C_TWO, 2, HY, HX), BF),
            jax.ShapeDtypeStruct((32, 16, HX), BF),
        ),
        in_specs=[SMEM] + [VMEM] * 8,
        out_specs=(HBM, VMEM),
        scratch_shapes=[
            pltpu.VMEM((C_IN * V_PITCH, HX), F32),
            pltpu.VMEM((48, 4 * CELLS), BF),
            pltpu.VMEM((96, 37 * HX), BF),
            pltpu.VMEM((192, 2 * CELLS), BF),
            pltpu.VMEM((192, 2 * CELLS), BF),
            pltpu.VMEM((C_TWO * C_PITCH, HX), F32),
            pltpu.VMEM((1, C_TWO, 2, HY, HX), BF),
            pltpu.VMEM((C_ONE, 4 * CELLS), F32),
            pltpu.VMEM((288, 2 * CELLS), F32),
            pltpu.SemaphoreType.DMA,
        ],
        compiler_params=pltpu.CompilerParams(vmem_limit_bytes=24 * 1024 * 1024),
        interpret=interpret,
        name="slab",
    )(depth, va, vb, *ready)


def split(total, interpret=False):
    return pl.pallas_call(
        unpack,
        out_shape=(
            jax.ShapeDtypeStruct((27, C_ONE, C_TWO), F32),
            jax.ShapeDtypeStruct((27, C_IN, C_ONE), F32),
            jax.ShapeDtypeStruct((1, C_ONE), F32),
            jax.ShapeDtypeStruct((1, C_TWO), F32),
        ),
        in_specs=[VMEM],
        out_specs=(VMEM,) * 4,
        compiler_params=pltpu.CompilerParams(vmem_limit_bytes=4 * 1024 * 1024),
        interpret=interpret,
        name="unpack",
    )(total)


def per_device(volume, kernel_one, bias_one, kernel_two, bias_two, cotangent):
    even, odd = swapped(volume, 0), swapped(volume, 1)
    depth = jnp.stack([lax.axis_index(DEPTH), lax.axis_size(DEPTH)]).astype(jnp.int32)
    w1 = jnp.transpose(kernel_one, (2, 3, 4, 1, 0)).reshape(27, C_IN, C_ONE)
    w2 = jnp.transpose(kernel_two, (2, 3, 4, 1, 0)).reshape(27, C_ONE, C_TWO)
    features, packed = local(depth, odd, volume, even, w1, bias_one[None], w2, bias_two[None], cotangent)
    two, one, b1, b2 = split(reduced(packed))
    two = jnp.transpose(two.reshape(3, 3, 3, C_ONE, C_TWO), (4, 3, 0, 1, 2))
    one = jnp.transpose(one.reshape(3, 3, 3, C_IN, C_ONE), (4, 3, 0, 1, 2))
    return (features, one, b1[0], two, b2[0])


def solution(mesh):
    cut = Mesh(mesh.devices.reshape(8, 2, 2, 4, 2), DP + DEPTH)
    return jax.shard_map(
        per_device,
        mesh=cut,
        in_specs=(
            P(DP, None, DEPTH, None, None),
            P(),
            P(),
            P(),
            P(),
            P(DP, None, DEPTH, None, None),
        ),
        out_specs=(P(DP, None, DEPTH, None, None), P(), P(), P(), P()),
        check_vma=False,
    )
```

```python
import jax
import jax.numpy as jnp
from jax import lax
from jax.experimental import pallas as pl
from jax.experimental.pallas import tpu as pltpu
from jax.sharding import Mesh
from jax.sharding import PartitionSpec as P

DP = ("z", "x_hi", "core")
DEPTH = ("y", "x_lo")
PLANE = ("x_hi", "core", "y", "x_lo")
LINE = ("z",)

BF = jnp.bfloat16
F32 = jnp.float32
HY = 8
HX = 128
CELLS = HY * HX
ROWS = HY + 1
C_IN = 4
C_ONE = 32
C_TWO = 64
STEP = 8
V_PITCH = 56
C_PITCH = 24


def dot_nn(a, b):
    return lax.dot_general(a, b, (((1,), (0,)), ((), ())), preferred_element_type=F32)


def dot_nt(a, b):
    return lax.dot_general(a, b, (((1,), (1,)), ((), ())), preferred_element_type=F32)


def identity(n):
    return lax.broadcasted_iota(jnp.int32, (n, n), 0) == lax.broadcasted_iota(jnp.int32, (n, n), 1)


def column(row):
    n = row.shape[1]
    return jnp.sum(jnp.where(identity(n), jnp.broadcast_to(row, (n, n)), 0.0), axis=1, keepdims=True)


def transposed(w):
    return dot_nt(identity(w.shape[1]).astype(BF), w).astype(BF)


def sigmoid(v):
    return 1.0 / (1.0 + jnp.exp(-v))


def neighbours(x):
    lane = lax.broadcasted_iota(jnp.int32, x.shape, 1)
    zero = jnp.zeros((), x.dtype)
    before = jnp.where(lane == 0, zero, pltpu.roll(x, 1, 1))
    after = jnp.where(lane == HX - 1, zero, pltpu.roll(x, HX - 1, 1))
    return before, x, after


def taps(to, p, load):
    last = jnp.where(lax.broadcasted_iota(jnp.int32, (4, HX), 0) == 0, 1.0, 0.0)
    edge = jnp.concatenate([jnp.zeros((12, HX), F32), last], axis=0).astype(BF)
    to[0:16, p * CELLS : p * CELLS + HX] = edge
    to[32:48, p * CELLS + 7 * HX : (p + 1) * CELLS] = edge
    for y in range(HY):
        before, slab, after = neighbours(load(y))
        moved = jnp.concatenate([before, slab, after, last], axis=0).astype(BF)
        for b in range(3):
            row = y + 1 - b
            if 0 <= row < HY:
                to[b * 16 : b * 16 + 16, p * CELLS + row * HX : p * CELLS + (row + 1) * HX] = moved


def prepare(
    v0, w1, b1, w2, b2, c0,
    own, w1t, w2t, flip, bias, cot,
    vv, w1v, w2v, cv, bv1, bv2, vs, w1s, cs, sems,
):
    copies = [
        pltpu.make_async_copy(src, dst, sems.at[n])
        for n, (src, dst) in enumerate(((w1, w1v), (w2, w2v), (b1, bv1), (b2, bv2), (c0, cv), (v0, vv)))
    ]
    for copy in copies:
        copy.start()
    w1s[...] = jnp.zeros((144, C_ONE), F32)
    copies[0].wait()
    for a in range(3):
        for t in range(9):
            row = a * 48 + t // 3 * 16 + t % 3 * 4
            w1s[row : row + 4, :] = w1v[a * 9 + t].astype(F32)
    w1t[...] = transposed(w1s[...].astype(BF))
    copies[1].wait()
    w2t[...] = transposed(w2v[...].reshape(864, C_TWO))
    for k in range(9):
        flip[k * C_ONE : (k + 1) * C_ONE, :] = jnp.concatenate([w2v[(8 - k) * 3 + 2 - c] for c in range(3)], axis=1)
    copies[2].wait()
    copies[3].wait()
    bias[0:C_ONE, :] = jnp.broadcast_to(column(bv1[...]), (C_ONE, HX))
    bias[C_ONE:, :] = jnp.broadcast_to(column(bv2[...]), (C_TWO, HX))
    copies[5].wait()
    for p in range(2):
        for i in range(C_IN):
            vs[i * V_PITCH + p * HY : i * V_PITCH + (p + 1) * HY, :] = vv[0, i, p].astype(F32)
    for p in range(2):
        taps(own, p, lambda y: vs[pl.ds(p * HY + y, C_IN, stride=V_PITCH), :])
    copies[4].wait()
    for o in range(C_TWO):
        for z in range(2):
            cs[o * C_PITCH + z * HY : o * C_PITCH + (z + 1) * HY, :] = cv[0, o, z].astype(F32)
    for row in range(2 * HY):
        cot[:, row * HX : (row + 1) * HX] = cs[pl.ds(row, C_TWO, stride=C_PITCH), :].astype(BF)


def compute(
    depth, va, vb, own, w1t, w2t, flip, bias, cot,
    features, packed,
    vs, x1b, x3, s3, sb, fs, fb, p1, rs, sem,
):
    even = depth[0] % 2 == 1
    for p in range(4):
        for i in range(C_IN):
            near = va[0, i, p % 2].astype(F32)
            far = vb[0, i, p % 2].astype(F32)
            plane = jnp.where(even, far, near) if p < 2 else jnp.where(even, near, far)
            vs[i * V_PITCH + p * HY : i * V_PITCH + (p + 1) * HY, :] = plane
    for p in range(4):
        taps(x1b, p, lambda y: vs[pl.ds(p * HY + y, C_IN, stride=V_PITCH), :])
    for p in range(5):
        x3[:, p * ROWS * HX : p * ROWS * HX + HX] = jnp.zeros((96, HX), BF)

    def planes(p):
        parts = []
        for q in (p, p + 1, p + 2):
            ref, at = (own, q - 2) if q in (2, 3) else (x1b, q if q < 2 else q - 2)
            parts.append(ref[:, at * CELLS : (at + 1) * CELLS])
        return jnp.concatenate(parts, axis=0)

    def first(p):
        pre = dot_nn(w1t[...], planes(p)) + bias[0:C_ONE, 0:1]
        sig = sigmoid(pre)
        act = pre * sig
        slope = sig + act * (1.0 - sig)
        if p in (0, 3):
            inside = jnp.where(depth[0] > 0 if p == 0 else depth[0] < depth[1] - 1, 1.0, 0.0)
            slope = slope * inside
            act = act * inside
        p1[:, p * CELLS : (p + 1) * CELLS] = slope
        for y in range(HY):
            col = (1 + p * ROWS + y) * HX
            for c, moved in enumerate(neighbours(act[:, y * HX : (y + 1) * HX].astype(BF))):
                x3[c * C_ONE : (c + 1) * C_ONE, col : col + HX] = moved

    def second(q):
        sb[0:C_TWO, q * CELLS + 7 * HX : (q + 1) * CELLS] = jnp.zeros((C_TWO, HX), BF)
        sb[2 * C_TWO :, q * CELLS : q * CELLS + HX] = jnp.zeros((C_TWO, HX), BF)
        for part in range(0, HY, STEP):
            cols = [((q + k // 3) * ROWS + k % 3 + part) * HX for k in range(9)]
            near = jnp.concatenate([x3[:, col : col + STEP * HX] for col in cols], axis=0)
            pre = dot_nn(w2t[...], near) + bias[C_ONE:, 0:1]
            sig = sigmoid(pre)
            act = pre * sig
            slope = sig + act * (1.0 - sig)
            for y in range(part, part + STEP):
                row = q * HY + y
                col = row * HX
                lane = (y - part) * HX
                up = cot[:, col : col + HX].astype(F32)
                here = (up * slope[:, lane : lane + HX]).astype(BF)
                for b in range(3):
                    to = y + b - 1
                    if 0 <= to < HY:
                        sb[b * C_TWO : (b + 1) * C_TWO, q * CELLS + to * HX : q * CELLS + (to + 1) * HX] = here
                for c, moved in enumerate(neighbours(here)):
                    s3[c * C_TWO : (c + 1) * C_TWO, col : col + HX] = moved
                fs[pl.ds(row, C_TWO, stride=C_PITCH), :] = act[:, lane : lane + HX]
        for o in range(C_TWO):
            fb[0, o, q] = fs[o * C_PITCH + q * HY : o * C_PITCH + (q + 1) * HY, :].astype(BF)

    def back(j):
        rs[:, j * CELLS : (j + 1) * CELLS] = dot_nn(flip[...], s3[:, j * CELLS : (j + 1) * CELLS])

    def two(j):
        near = [x3[:, (1 + (j + a) * ROWS) * HX : (1 + (j + a) * ROWS) * HX + CELLS] for a in range(3)]
        near = jnp.concatenate(near + [jnp.ones((16, CELLS), BF)], axis=0)
        return dot_nt(near, sb[:, j * CELLS : (j + 1) * CELLS])

    first(0)
    first(1)
    first(2)
    first(3)
    second(0)
    second(1)
    back(0)
    back(1)
    two_0 = two(0)
    two_1 = two(1)
    out = pltpu.make_async_copy(fb, features, sem)
    out.start()
    twos = two_0 + two_1
    grads = 0.0
    for t in range(4):
        shares = []
        for y in range(HY):
            total = 0.0
            for k in range(9):
                j, row = t + k // 3 - 2, y + k % 3 - 1
                if 0 <= j < 2 and 0 <= row < HY:
                    col = j * CELLS + row * HX
                    total = total + rs[k * C_ONE : (k + 1) * C_ONE, col : col + HX]
            shares.append(total * p1[:, t * CELLS + y * HX : t * CELLS + (y + 1) * HX])
        share = jnp.concatenate(shares, axis=1)
        high = share.astype(BF)
        share = jnp.concatenate([high, (share - high.astype(F32)).astype(BF)], axis=0)
        grads = grads + dot_nt(planes(t), share)
    grads = grads[:, :C_ONE] + grads[:, C_ONE:]
    side = twos[:, 2 * C_TWO :]
    third = jnp.concatenate([grads[96:], jnp.zeros((48, C_ONE), F32)], axis=0)
    rows = jnp.concatenate(
        [
            twos[:288, : 2 * C_TWO],
            jnp.concatenate([side[:96], side[96:192]], axis=1),
            jnp.concatenate([side[192:288], grads[:96], third], axis=1),
            twos[288:, : 2 * C_TWO],
            jnp.zeros((16, HX), F32),
        ],
        axis=0,
    )
    packed[...] = rows.astype(BF).reshape(32, 16, HX)
    out.wait()


def place(k):
    a, b = k // 3, k % 3
    if b < 2:
        return a * 96, b * C_TWO
    return (288, a * C_TWO) if a < 2 else (384, 0)


def place_one(a):
    return 384 + a % 2 * 48, C_TWO + a // 2 * C_ONE


def unpack(total, out, one, bias_one, bias_two, two, sems):
    flat = total[...].astype(F32).reshape(512, HX)
    copies = []
    for k in range(9):
        r, lane = place(k)
        two[3 * k : 3 * k + 3] = flat[r : r + 96, lane : lane + 64].reshape(3, C_ONE, C_TWO)
        if k % 3 == 2:
            part = pl.ds(9 * (k // 3), 9)
            copies.append(pltpu.make_async_copy(two.at[part], out.at[part], sems.at[k // 3]))
            copies[-1].start()
    for a in range(3):
        r, lane = place_one(a)
        for t in range(9):
            row = r + t // 3 * 16 + t % 3 * 4
            one[a * 9 + t] = flat[row : row + 4, lane : lane + C_ONE]
    bias_one[...] = flat[384 + 12 : 384 + 13, C_TWO : C_TWO + C_ONE]
    bias_two[...] = flat[480:481, C_TWO : 2 * C_TWO]
    for copy in copies:
        copy.wait()


def exchange(x, axes, first):
    order = [first] + [i for i in range(lax.axis_size(axes)) if i != first]
    return lax.all_to_all(x, axes, 0, 0, axis_index_groups=[order], tiled=True)


def middle(axes):
    index = 0
    for axis in axes:
        size = lax.axis_size(axis)
        index = index * size + {"x_hi": 1, "x_lo": 0, "core": 1}.get(axis, size // 2)
    return index


def reduced(x):
    plane = lax.axis_size(PLANE)
    line = lax.axis_size(LINE)
    part = exchange(x, PLANE, middle(PLANE))
    part = jnp.sum(part, axis=0, dtype=F32).astype(x.dtype)
    part = exchange(jnp.broadcast_to(part[None], (line,) + part.shape), LINE, middle(LINE))
    part = jnp.sum(part, axis=0, dtype=F32).astype(x.dtype)
    return exchange(jnp.broadcast_to(part[None], (plane,) + part.shape), PLANE, middle(PLANE))


def swapped(x, first):
    size = lax.axis_size(DEPTH)
    ups = [(i, i + 1) for i in range(first, size - 1, 2)]
    return lax.ppermute(x, DEPTH, ups + [(j, i) for i, j in ups])


VMEM = pl.BlockSpec(memory_space=pltpu.VMEM)
HBM = pl.BlockSpec(memory_space=pltpu.HBM)
SMEM = pl.BlockSpec(memory_space=pltpu.SMEM)


def local(depth, va, v0, vb, w1, b1, w2, b2, cot, interpret=False):
    held = [x if interpret else pltpu.with_memory_space_constraint(x, pltpu.HBM) for x in (v0, w1, b1, w2, b2, cot)]
    ready = pl.pallas_call(
        prepare,
        out_shape=(
            jax.ShapeDtypeStruct((48, 2 * CELLS), BF),
            jax.ShapeDtypeStruct((C_ONE, 144), BF),
            jax.ShapeDtypeStruct((C_TWO, 864), BF),
            jax.ShapeDtypeStruct((288, 192), BF),
            jax.ShapeDtypeStruct((96, HX), F32),
            jax.ShapeDtypeStruct((C_TWO, 2 * CELLS), BF),
        ),
        in_specs=[HBM] * 6,
        out_specs=(VMEM,) * 6,
        scratch_shapes=[
            pltpu.VMEM((1, C_IN, 2, HY, HX), BF),
            pltpu.VMEM((27, C_IN, C_ONE), BF),
            pltpu.VMEM((27, C_ONE, C_TWO), BF),
            pltpu.VMEM((1, C_TWO, 2, HY, HX), BF),
            pltpu.VMEM((1, C_ONE), F32),
            pltpu.VMEM((1, C_TWO), F32),
            pltpu.VMEM((C_IN * V_PITCH, HX), F32),
            pltpu.VMEM((144, C_ONE), F32),
            pltpu.VMEM((C_TWO * C_PITCH, HX), F32),
            pltpu.SemaphoreType.DMA((6,)),
        ],
        compiler_params=pltpu.CompilerParams(vmem_limit_bytes=16 * 1024 * 1024),
        interpret=interpret,
        name="prepare",
    )(*held)
    return pl.pallas_call(
        compute,
        out_shape=(
            jax.ShapeDtypeStruct((1, C_TWO, 2, HY, HX), BF),
            jax.ShapeDtypeStruct((32, 16, HX), BF),
        ),
        in_specs=[SMEM] + [VMEM] * 8,
        out_specs=(HBM, VMEM),
        scratch_shapes=[
            pltpu.VMEM((C_IN * V_PITCH, HX), F32),
            pltpu.VMEM((48, 4 * CELLS), BF),
            pltpu.VMEM((96, 37 * HX), BF),
            pltpu.VMEM((192, 2 * CELLS), BF),
            pltpu.VMEM((192, 2 * CELLS), BF),
            pltpu.VMEM((C_TWO * C_PITCH, HX), F32),
            pltpu.VMEM((1, C_TWO, 2, HY, HX), BF),
            pltpu.VMEM((C_ONE, 4 * CELLS), F32),
            pltpu.VMEM((288, 2 * CELLS), F32),
            pltpu.SemaphoreType.DMA,
        ],
        compiler_params=pltpu.CompilerParams(vmem_limit_bytes=24 * 1024 * 1024),
        interpret=interpret,
        name="slab",
    )(depth, va, vb, *ready)


def split(total, interpret=False):
    return pl.pallas_call(
        unpack,
        out_shape=(
            jax.ShapeDtypeStruct((27, C_ONE, C_TWO), F32),
            jax.ShapeDtypeStruct((27, C_IN, C_ONE), F32),
            jax.ShapeDtypeStruct((1, C_ONE), F32),
            jax.ShapeDtypeStruct((1, C_TWO), F32),
        ),
        in_specs=[VMEM],
        out_specs=(HBM, VMEM, VMEM, VMEM),
        scratch_shapes=[pltpu.VMEM((27, C_ONE, C_TWO), F32), pltpu.SemaphoreType.DMA((3,))],
        compiler_params=pltpu.CompilerParams(vmem_limit_bytes=4 * 1024 * 1024),
        interpret=interpret,
        name="unpack",
    )(total)


def per_device(volume, kernel_one, bias_one, kernel_two, bias_two, cotangent):
    even, odd = swapped(volume, 0), swapped(volume, 1)
    depth = jnp.stack([lax.axis_index(DEPTH), lax.axis_size(DEPTH)]).astype(jnp.int32)
    w1 = jnp.transpose(kernel_one, (2, 3, 4, 1, 0)).reshape(27, C_IN, C_ONE)
    w2 = jnp.transpose(kernel_two, (2, 3, 4, 1, 0)).reshape(27, C_ONE, C_TWO)
    features, packed = local(depth, odd, volume, even, w1, bias_one[None], w2, bias_two[None], cotangent)
    two, one, b1, b2 = split(reduced(packed))
    two = jnp.transpose(two.reshape(3, 3, 3, C_ONE, C_TWO), (4, 3, 0, 1, 2))
    one = jnp.transpose(one.reshape(3, 3, 3, C_IN, C_ONE), (4, 3, 0, 1, 2))
    return (features, one, b1[0], two, b2[0])


def solution(mesh):
    cut = Mesh(mesh.devices.reshape(8, 2, 2, 4, 2), DP + DEPTH)
    return jax.shard_map(
        per_device,
        mesh=cut,
        in_specs=(
            P(DP, None, DEPTH, None, None),
            P(),
            P(),
            P(),
            P(),
            P(DP, None, DEPTH, None, None),
        ),
        out_specs=(P(DP, None, DEPTH, None, None), P(), P(), P(), P()),
        check_vma=False,
    )
```
